8 devices in a mesh: stage: 1 (over z), model: 2 (over y), data: 4 (over x, core).
Axes of the slice: x: 2, y: 2, z: 1, core: 2. Of those that a mesh axis runs over, the one named last changes fastest.
Arguments:
- w_fc1: float32 [32, 1536, 1024], P('stage', 'data', 'model')
- m_fc1: float32 [32, 1536, 1024], P('stage', 'data', 'model')
- g_fc1: bfloat16 [32, 1536, 1024], P('stage', 'data', 'model')
- w_fc2: float32 [32, 1536, 512], P('stage', 'data', 'model')
- m_fc2: float32 [32, 1536, 512], P('stage', 'data', 'model')
- g_fc2: bfloat16 [32, 1536, 512], P('stage', 'data', 'model')
Outputs:
- output 1: float32 [32, 1536, 1024], P('stage', 'data', 'model')
- output 2: float32 [32, 1536, 1024], P('stage', 'data', 'model')
- output 3: float32 [32, 1536, 512], P('stage', 'data', 'model')
- output 4: float32 [32, 1536, 512], P('stage', 'data', 'model')
All inputs are finite; a program needn't handle non-finite values.
Results may differ from the reference program's by a relative error of at most 0.00830859.
Values are sent between devices in bfloat16 or wider.
A program may use at most 1 GiB of HBM per device.

```python
import math
import jax
import jax.numpy as jnp
from jax import lax

HIDDEN = 1536
EXPERT_FFN = 512
EXPERTS = 32
NS_STEPS = 5
LOW_RANK = 4

NS_COEF_A = 3.4445
NS_COEF_B = -4.7750
NS_COEF_C = 2.0315
MOMENTUM = 0.95
LEARN_RATE = 0.04
DECAY = 0.2
NORM_EPS = 1e-7


def draw_state(key, cols):
    key_noise, key_left, key_right, key_scale = jax.random.split(key, 4)
    noise = jax.random.normal(key_noise, (EXPERTS, HIDDEN, cols), jnp.float32)
    left = jax.random.normal(key_left, (EXPERTS, HIDDEN, LOW_RANK), jnp.float32)
    right = jax.random.normal(key_right, (EXPERTS, LOW_RANK, cols), jnp.float32)
    shared = jnp.einsum('emr,ern->emn', left, right) / math.sqrt(LOW_RANK)
    row_scale = jax.random.uniform(key_scale, (EXPERTS, HIDDEN, 1), jnp.float32, 0.5, 1.5)
    return row_scale * (noise + shared) * math.sqrt(0.5)


def setup_inputs(seed: int = 0, part: int = 0) -> dict:
    base = jax.random.fold_in(jax.random.key(seed), part)
    keys = jax.random.split(base, 6)
    fc1_cols = 2 * EXPERT_FFN
    w_scale = HIDDEN ** -0.5
    return {
        'w_fc1': jax.random.normal(keys[0], (EXPERTS, HIDDEN, fc1_cols), jnp.float32) * w_scale,
        'm_fc1': draw_state(keys[1], fc1_cols),
        'g_fc1': draw_state(keys[2], fc1_cols).astype(jnp.bfloat16),
        'w_fc2': jax.random.normal(keys[3], (EXPERTS, HIDDEN, EXPERT_FFN), jnp.float32) * w_scale,
        'm_fc2': draw_state(keys[4], EXPERT_FFN),
        'g_fc2': draw_state(keys[5], EXPERT_FFN).astype(jnp.bfloat16),
    }


def orthogonalize(momentum):
    row_count, col_count = momentum.shape
    norm_val = jnp.sqrt(jnp.sum(momentum * momentum))
    x_mat = (momentum.astype(jnp.bfloat16).astype(jnp.float32) / (norm_val + NORM_EPS)).astype(jnp.bfloat16)
    if row_count > col_count:
        x_mat = x_mat.T
    for ns_step in range(NS_STEPS):
        gram_mat = jnp.dot(x_mat, x_mat.T, preferred_element_type=jnp.float32).astype(jnp.bfloat16)
        gram_sq = jnp.dot(gram_mat, gram_mat, preferred_element_type=jnp.float32)
        poly_mat = (NS_COEF_B * gram_mat.astype(jnp.float32) + NS_COEF_C * gram_sq).astype(jnp.bfloat16)
        update_term = jnp.dot(poly_mat, x_mat, preferred_element_type=jnp.float32)
        x_mat = (NS_COEF_A * x_mat.astype(jnp.float32) + update_term).astype(jnp.bfloat16)
    if row_count > col_count:
        x_mat = x_mat.T
    return x_mat.astype(jnp.float32) * (0.2 * math.sqrt(max(row_count, col_count)))


def update_stack(weights, momentum, gradient):
    new_mom = MOMENTUM * momentum + gradient.astype(jnp.float32)
    ortho = lax.map(orthogonalize, new_mom)
    new_w = weights - LEARN_RATE * (ortho + DECAY * weights)
    return new_w, new_mom


def reference(w_fc1, m_fc1, g_fc1, w_fc2, m_fc2, g_fc2):
    new_w1, new_m1 = update_stack(w_fc1, m_fc1, g_fc1)
    new_w2, new_m2 = update_stack(w_fc2, m_fc2, g_fc2)
    return (new_w1, new_m1, new_w2, new_m2)
```

```python
import functools
import math
import jax
import jax.numpy as jnp
from jax import lax
from jax.experimental import pallas as pl
from jax.experimental.pallas import tpu as pltpu
from jax.sharding import PartitionSpec as P

NS_STEPS = 5
NS_COEF_A = 3.4445
NS_COEF_B = -4.7750
NS_COEF_C = 2.0315
MOMENTUM = 0.95
LEARN_RATE = 0.04
DECAY = 0.2
NORM_EPS = 1e-7

MESH_ID = pl.DeviceIdType.MESH
GRAM_BLOCK = 256
ROW_BLOCK = 512


def momentum_kernel(m_ref, g_ref, new_m_ref, low_ref, sq_ref):
    new_mom = MOMENTUM * m_ref[0] + g_ref[0].astype(jnp.float32)
    new_m_ref[0] = new_mom
    low_ref[0] = new_mom.astype(jnp.bfloat16)
    squares = new_mom * new_mom
    rows, cols = squares.shape
    part = jnp.sum(squares.reshape(rows // 8, 8, cols), axis=0)
    total = part[:, :128]
    for start in range(128, cols, 128):
        total = total + part[:, start:start + 128]
    sq_ref[0, 0] = total


def momentum_step(m_loc, g_loc, owners):
    experts, rows, cols = m_loc.shape
    rounds = experts // owners
    block = pl.BlockSpec((1, rows, cols), lambda e: (e, 0, 0))
    return pl.pallas_call(
        momentum_kernel,
        grid=(experts,),
        in_specs=[block, block],
        out_specs=[block, block, pl.BlockSpec((1, 1, 8, 128), lambda e: (e % owners, e // owners, 0, 0))],
        out_shape=[
            jax.ShapeDtypeStruct(m_loc.shape, jnp.float32),
            jax.ShapeDtypeStruct(m_loc.shape, jnp.bfloat16),
            jax.ShapeDtypeStruct((owners, rounds, 8, 128), jnp.float32),
        ],
        compiler_params=pltpu.CompilerParams(dimension_semantics=('arbitrary',), vmem_limit_bytes=32 * 2 ** 20),
        name='momentum',
    )(m_loc, g_loc)


def iterate(x_ref, gram_ref, poly_ref):
    rows, cols = x_ref.shape
    gram_block = min(GRAM_BLOCK, cols)
    row_block = min(ROW_BLOCK, rows)

    @pl.loop(0, NS_STEPS)
    def ns_step(_):
        @pl.loop(0, cols // gram_block)
        def gram(i):
            span = pl.ds(pl.multiple_of(i * gram_block, gram_block), gram_block)
            part = lax.dot_general(x_ref[:, span], x_ref[...], (((0,), (0,)), ((), ())), preferred_element_type=jnp.float32)
            gram_ref[span, :] = part.astype(jnp.bfloat16)

        @pl.loop(0, cols // gram_block)
        def poly(i):
            span = pl.ds(pl.multiple_of(i * gram_block, gram_block), gram_block)
            gram_rows = gram_ref[span, :]
            gram_sq = jnp.dot(gram_rows, gram_ref[...], preferred_element_type=jnp.float32)
            poly_ref[span, :] = (NS_COEF_B * gram_rows.astype(jnp.float32) + NS_COEF_C * gram_sq).astype(jnp.bfloat16)

        @pl.loop(0, rows // row_block)
        def update(i):
            span = pl.ds(pl.multiple_of(i * row_block, row_block), row_block)
            x_rows = x_ref[span, :]
            term = jnp.dot(x_rows, poly_ref[...], preferred_element_type=jnp.float32)
            x_ref[span, :] = (NS_COEF_A * x_rows.astype(jnp.float32) + term).astype(jnp.bfloat16)


def exchange_kernel(low1, low2, sq1, sq2, back1, back2, x1, x2, sums1, sums2, gram1, poly1, gram2, poly2,
                    fwd1, fwd2, got1, got2, ret1, ret2, done_sems, sq_send, sq_got):
    model = lax.axis_index('model')
    data = lax.axis_index('data')
    chip, core = data // 2, data % 2
    me = model * 4 + data
    owners = 8
    rounds = low1.shape[0] // owners

    offsets = [(1, 0, 0), (0, 1, 0), (1, 0, 1), (0, 1, 1), (1, 1, 0), (1, 1, 1), (0, 0, 1)]
    others = [((model + dm) % 2, ((chip + dx) % 2) * 2 + (core + dc) % 2) for dm, dx, dc in offsets]

    barrier = pltpu.get_barrier_semaphore()
    for peer_model, peer_data in others:
        pl.semaphore_signal(barrier, inc=1, device_id=(0, peer_model, peer_data), device_id_type=MESH_ID)
    pl.semaphore_wait(barrier, len(others))

    def window(x_ref, k, at_model, at_data):
        rows, cols = x_ref.shape[1] // 4, x_ref.shape[2] // 2
        return x_ref.at[k, pl.ds(pl.multiple_of(at_data * rows, rows), rows), pl.ds(pl.multiple_of(at_model * cols, cols), cols)]

    for src, dst, t in ((sq2, sums2, 0), (sq1, sums1, 1)):
        for peer_model, peer_data in others:
            pltpu.make_async_remote_copy(src.at[peer_model * 4 + peer_data], dst.at[me], sq_send.at[t], sq_got.at[t],
                                         device_id=(0, peer_model, peer_data), device_id_type=MESH_ID).start()
        pltpu.make_async_copy(src.at[me], dst.at[me], sq_got.at[t]).start()

    def send_round(k):
        for src, x_ref, sems, got in ((low2, x2, fwd2, got2), (low1, x1, fwd1, got1)):
            for peer_model, peer_data in others:
                pltpu.make_async_remote_copy(src.at[k * owners + peer_model * 4 + peer_data], window(x_ref, k, model, data),
                                             sems.at[k], got.at[k],
                                             device_id=(0, peer_model, peer_data), device_id_type=MESH_ID).start()
            pltpu.make_async_copy(src.at[k * owners + me], window(x_ref, k, model, data), got.at[k]).start()

    def return_round(k, x_ref, dst, sems, t):
        for peer_model, peer_data in others:
            pltpu.make_async_remote_copy(window(x_ref, k, peer_model, peer_data), dst.at[k * owners + me],
                                         sems.at[k], done_sems.at[t],
                                         device_id=(0, peer_model, peer_data), device_id_type=MESH_ID).start()
        pltpu.make_async_copy(window(x_ref, k, model, data), dst.at[k * owners + me], done_sems.at[t]).start()

    def wait_bytes(ref, sem):
        pltpu.make_async_copy(ref, ref, sem).wait()

    def orthogonalize(k, x_ref, sums_ref, gram_ref, poly_ref):
        norm = jnp.sqrt(jnp.sum(sums_ref[:, k])) + NORM_EPS
        rows = x_ref.shape[1]

        @pl.loop(0, rows // 256)
        def normalize(i):
            span = pl.ds(pl.multiple_of(i * 256, 256), 256)
            x_ref[k, span, :] = (x_ref[k, span, :].astype(jnp.float32) / norm).astype(jnp.bfloat16)

        iterate(x_ref.at[k], gram_ref, poly_ref)

    @pl.loop(0, rounds)
    def forward(k):
        send_round(k)

    wait_bytes(sums2, sq_got.at[0])
    wait_bytes(sums1, sq_got.at[1])

    @pl.loop(0, rounds)
    def work(k):
        wait_bytes(x2.at[k], got2.at[k])
        orthogonalize(k, x2, sums2, gram2, poly2)
        return_round(k, x2, back2, ret2, 0)
        wait_bytes(x1.at[k], got1.at[k])
        orthogonalize(k, x1, sums1, gram1, poly1)
        return_round(k, x1, back1, ret1, 1)

    for src, t in ((sq2, 0), (sq1, 1)):
        wait_bytes(src.at[pl.ds(0, len(others))], sq_send.at[t])

    @pl.loop(0, rounds)
    def finish(k):
        for low, fwd, ret in ((low2, fwd2, ret2), (low1, fwd1, ret1)):
            sent = low.at[pl.ds(0, len(others))]
            wait_bytes(sent, fwd.at[k])
            wait_bytes(sent, ret.at[k])

    wait_bytes(back2, done_sems.at[0])
    wait_bytes(back1, done_sems.at[1])


def exchange(low1, low2, sq1, sq2):
    owners, rounds = sq1.shape[:2]
    _, rows1, cols1 = low1.shape
    _, rows2, cols2 = low2.shape
    any_spec = pl.BlockSpec(memory_space=pl.ANY)
    flops = 2 * rounds * NS_STEPS * sum(2 * 4 * r * (2 * c) ** 2 + (2 * c) ** 3 for r, c in ((rows1, cols1), (rows2, cols2)))
    dma = pltpu.SemaphoreType.DMA
    return pl.pallas_call(
        exchange_kernel,
        in_specs=[any_spec] * 4,
        out_specs=[any_spec] * 2,
        out_shape=[jax.ShapeDtypeStruct(low1.shape, low1.dtype), jax.ShapeDtypeStruct(low2.shape, low2.dtype)],
        scratch_shapes=[
            pltpu.VMEM((rounds, 4 * rows1, 2 * cols1), jnp.bfloat16),
            pltpu.VMEM((rounds, 4 * rows2, 2 * cols2), jnp.bfloat16),
            pltpu.VMEM((owners, rounds, 8, 128), jnp.float32),
            pltpu.VMEM((owners, rounds, 8, 128), jnp.float32),
            pltpu.VMEM((2 * cols1, 2 * cols1), jnp.bfloat16),
            pltpu.VMEM((2 * cols1, 2 * cols1), jnp.bfloat16),
            pltpu.VMEM((2 * cols2, 2 * cols2), jnp.bfloat16),
            pltpu.VMEM((2 * cols2, 2 * cols2), jnp.bfloat16),
            dma((rounds,)), dma((rounds,)), dma((rounds,)), dma((rounds,)), dma((rounds,)), dma((rounds,)),
            dma((2,)), dma((2,)), dma((2,)),
        ],
        compiler_params=pltpu.CompilerParams(collective_id=0, has_side_effects=True, vmem_limit_bytes=56 * 2 ** 20),
        cost_estimate=pl.CostEstimate(flops=flops, bytes_accessed=4 * (low1.size + low2.size), transcendentals=0),
        name='exchange',
    )(low1, low2, sq1, sq2)


def weight_step(w_loc, x_back, rows_full, cols_full):
    step_scale = 0.2 * math.sqrt(max(rows_full, cols_full))
    return w_loc - LEARN_RATE * (x_back.astype(jnp.float32) * step_scale + DECAY * w_loc)


def solution(mesh):
    data_size = mesh.shape['data']
    model_size = mesh.shape['model']
    owners = data_size * model_size
    block_spec = P('stage', 'data', 'model')

    def local_step(w_fc1, m_fc1, g_fc1, w_fc2, m_fc2, g_fc2):
        new_m2, low2, sq2 = momentum_step(m_fc2, g_fc2, owners)
        new_m1, low1, sq1 = momentum_step(m_fc1, g_fc1, owners)
        back1, back2 = exchange(low1, low2, sq1, sq2)
        full = [(w.shape[1] * data_size, w.shape[2] * model_size) for w in (w_fc1, w_fc2)]
        new_w1 = weight_step(w_fc1, back1, *full[0])
        new_w2 = weight_step(w_fc2, back2, *full[1])
        return new_w1, new_m1, new_w2, new_m2

    return jax.shard_map(local_step, mesh=mesh, in_specs=(block_spec,) * 6, out_specs=(block_spec,) * 4, check_vma=False)
```

```python
import functools
import math
import jax
import jax.numpy as jnp
from jax import lax
from jax.experimental import pallas as pl
from jax.experimental.pallas import tpu as pltpu
from jax.sharding import PartitionSpec as P

NS_STEPS = 5
NS_COEF_A = 3.4445
NS_COEF_B = -4.7750
NS_COEF_C = 2.0315
MOMENTUM = 0.95
LEARN_RATE = 0.04
DECAY = 0.2
NORM_EPS = 1e-7

MESH_ID = pl.DeviceIdType.MESH
GRAM_BLOCK = 256
ROW_BLOCK = 512


def iterate(x_ref, gram_ref, poly_ref):
    rows, cols = x_ref.shape
    gram_block = min(GRAM_BLOCK, cols)
    row_block = min(ROW_BLOCK, rows)

    @pl.loop(0, NS_STEPS)
    def ns_step(_):
        @pl.loop(0, cols // gram_block)
        def gram(i):
            span = pl.ds(pl.multiple_of(i * gram_block, gram_block), gram_block)
            part = lax.dot_general(x_ref[:, span], x_ref[...], (((0,), (0,)), ((), ())), preferred_element_type=jnp.float32)
            gram_ref[span, :] = part.astype(jnp.bfloat16)

        @pl.loop(0, cols // gram_block)
        def poly(i):
            span = pl.ds(pl.multiple_of(i * gram_block, gram_block), gram_block)
            gram_rows = gram_ref[span, :]
            gram_sq = jnp.dot(gram_rows, gram_ref[...], preferred_element_type=jnp.float32)
            poly_ref[span, :] = (NS_COEF_B * gram_rows.astype(jnp.float32) + NS_COEF_C * gram_sq).astype(jnp.bfloat16)

        @pl.loop(0, rows // row_block)
        def update(i):
            span = pl.ds(pl.multiple_of(i * row_block, row_block), row_block)
            x_rows = x_ref[span, :]
            term = jnp.dot(x_rows, poly_ref[...], preferred_element_type=jnp.float32)
            x_ref[span, :] = (NS_COEF_A * x_rows.astype(jnp.float32) + term).astype(jnp.bfloat16)


def momentum_block(m_ref, g_ref, slot, low_ref, index, sq_ref, owner, k):
    new_mom = MOMENTUM * m_ref[slot] + g_ref[slot].astype(jnp.float32)
    low_ref[index] = new_mom.astype(jnp.bfloat16)
    squares = new_mom * new_mom
    rows, cols = squares.shape
    part = jnp.sum(squares.reshape(rows // 8, 8, cols), axis=0)
    total = part[:, :128]
    for start in range(128, cols, 128):
        total = total + part[:, start:start + 128]
    sq_ref[owner, k] = total


def exchange_kernel(m1, g1, m2, g2, back1, back2, last, low1, low2, x1, x2, sq1, sq2, sums1, sums2,
                    gram1, poly1, gram2, poly2, m_buf1, g_buf1, m_buf2, g_buf2,
                    fwd1, fwd2, got1, got2, ret1, ret2, done_sems, sq_send1, sq_send2, sq_got1, sq_got2,
                    m_sem1, g_sem1, m_sem2, g_sem2, last_sem):
    model = lax.axis_index('model')
    data = lax.axis_index('data')
    chip, core = data // 2, data % 2
    me = model * 4 + data
    owners = 8
    experts = m1.shape[0]
    rounds = experts // owners
    slots = m_buf1.shape[0]

    offsets = [(1, 0, 0), (0, 1, 0), (1, 0, 1), (0, 1, 1), (1, 1, 0), (1, 1, 1), (0, 0, 1)]
    others = [((model + dm) % 2, ((chip + dx) % 2) * 2 + (core + dc) % 2) for dm, dx, dc in offsets]

    def loads(m, g, m_buf, g_buf, m_sem, g_sem, index):
        slot = index % slots
        return (pltpu.make_async_copy(m.at[index], m_buf.at[slot], m_sem.at[slot]),
                pltpu.make_async_copy(g.at[index], g_buf.at[slot], g_sem.at[slot]))

    stack1 = (m1, g1, m_buf1, g_buf1, m_sem1, g_sem1)
    stack2 = (m2, g2, m_buf2, g_buf2, m_sem2, g_sem2)
    for stack in (stack2, stack1):
        for index in range(slots):
            for load in loads(*stack, index):
                load.start()

    barrier = pltpu.get_barrier_semaphore()
    for peer_model, peer_data in others:
        pl.semaphore_signal(barrier, inc=1, device_id=(0, peer_model, peer_data), device_id_type=MESH_ID)
    pl.semaphore_wait(barrier, len(others))

    def window(x_ref, k, at_model, at_data):
        rows, cols = x_ref.shape[1] // 4, x_ref.shape[2] // 2
        return x_ref.at[k, pl.ds(pl.multiple_of(at_data * rows, rows), rows), pl.ds(pl.multiple_of(at_model * cols, cols), cols)]

    def momentum_round(k, stack, low_ref, sq_ref):
        @pl.loop(0, owners)
        def block(owner):
            index = k * owners + owner
            for load in loads(*stack, index):
                load.wait()
            momentum_block(stack[2], stack[3], index % slots, low_ref, index, sq_ref, owner, k)

            @pl.when(index + slots < experts)
            def prefetch():
                for load in loads(*stack, index + slots):
                    load.start()

    def send_round(k, low_ref, x_ref, fwd, got, sq_ref, sums_ref, sq_send, sq_got):
        for peer_model, peer_data in others:
            owner = peer_model * 4 + peer_data
            to_owner = dict(device_id=(0, peer_model, peer_data), device_id_type=MESH_ID)
            pltpu.make_async_remote_copy(sq_ref.at[owner, k], sums_ref.at[k, me], sq_send.at[k], sq_got.at[k], **to_owner).start()
            pltpu.make_async_remote_copy(low_ref.at[k * owners + owner], window(x_ref, k, model, data), fwd.at[k], got.at[k],
                                         **to_owner).start()
        pltpu.make_async_copy(sq_ref.at[me, k], sums_ref.at[k, me], sq_got.at[k]).start()
        pltpu.make_async_copy(low_ref.at[k * owners + me], window(x_ref, k, model, data), got.at[k]).start()

    def return_round(k, x_ref, dst, sems, t, columns):
        @pl.when(k < rounds - 1)
        def to_holders():
            for peer_model, peer_data in others:
                pltpu.make_async_remote_copy(window(x_ref, k, peer_model, peer_data), dst.at[k * owners + me],
                                             sems.at[k], done_sems.at[t],
                                             device_id=(0, peer_model, peer_data), device_id_type=MESH_ID).start()
            pltpu.make_async_copy(window(x_ref, k, model, data), dst.at[k * owners + me], done_sems.at[t]).start()

        @pl.when(k == rounds - 1)
        def to_last():
            for holder in range(owners):
                pltpu.make_async_copy(window(x_ref, k, holder // 4, holder % 4), last.at[holder, :, columns], last_sem.at[t]).start()

    def wait_bytes(ref, sem):
        pltpu.make_async_copy(ref, ref, sem).wait()

    def orthogonalize(k, x_ref, got, sums_ref, sq_got, gram_ref, poly_ref):
        wait_bytes(sums_ref.at[k], sq_got.at[k])
        wait_bytes(x_ref.at[k], got.at[k])
        norm = jnp.sqrt(jnp.sum(sums_ref[k])) + NORM_EPS
        rows = x_ref.shape[1]

        @pl.loop(0, rows // 256)
        def normalize(i):
            span = pl.ds(pl.multiple_of(i * 256, 256), 256)
            x_ref[k, span, :] = (x_ref[k, span, :].astype(jnp.float32) / norm).astype(jnp.bfloat16)

        iterate(x_ref.at[k], gram_ref, poly_ref)

    @pl.loop(0, rounds)
    def forward(k):
        momentum_round(k, stack2, low2, sq2)
        send_round(k, low2, x2, fwd2, got2, sq2, sums2, sq_send2, sq_got2)
        momentum_round(k, stack1, low1, sq1)
        send_round(k, low1, x1, fwd1, got1, sq1, sums1, sq_send1, sq_got1)

    cols1, cols2 = low1.shape[2], low2.shape[2]

    @pl.loop(0, rounds)
    def work(k):
        orthogonalize(k, x2, got2, sums2, sq_got2, gram2, poly2)
        return_round(k, x2, back2, ret2, 0, pl.ds(cols1, cols2))
        orthogonalize(k, x1, got1, sums1, sq_got1, gram1, poly1)
        return_round(k, x1, back1, ret1, 1, pl.ds(0, cols1))

    count = len(others)

    @pl.loop(0, rounds)
    def finish(k):
        for low, sq, fwd, ret, sq_send in ((low2, sq2, fwd2, ret2, sq_send2), (low1, sq1, fwd1, ret1, sq_send1)):
            wait_bytes(sq.at[pl.ds(0, count), 0], sq_send.at[k])
            wait_bytes(low.at[pl.ds(0, count)], fwd.at[k])

            @pl.when(k < rounds - 1)
            def returned():
                wait_bytes(low.at[pl.ds(0, count)], ret.at[k])

    wait_bytes(back2, done_sems.at[0])
    wait_bytes(back1, done_sems.at[1])
    wait_bytes(last.at[:, :, pl.ds(cols1, cols2)], last_sem.at[0])
    wait_bytes(last.at[:, :, pl.ds(0, cols1)], last_sem.at[1])


def exchange(m1, g1, m2, g2, owners):
    experts, rows, cols1 = m1.shape
    cols2 = m2.shape[2]
    rounds = experts // owners
    slots = 4
    any_spec = pl.BlockSpec(memory_space=pl.ANY)
    flops = 2 * rounds * NS_STEPS * sum(2 * 4 * rows * c * c + c ** 3 for c in (2 * cols1, 2 * cols2))
    low = jnp.bfloat16
    dma = pltpu.SemaphoreType.DMA
    held = [jax.ShapeDtypeStruct((experts - owners, rows, c), low) for c in (cols1, cols2)]
    return pl.pallas_call(
        exchange_kernel,
        in_specs=[any_spec] * 4,
        out_specs=[any_spec] * 3,
        out_shape=held + [jax.ShapeDtypeStruct((owners, rows, cols1 + cols2), low)],
        scratch_shapes=[
            pltpu.VMEM((experts, rows, cols1), low),
            pltpu.VMEM((experts, rows, cols2), low),
            pltpu.VMEM((rounds, 4 * rows, 2 * cols1), low),
            pltpu.VMEM((rounds, 4 * rows, 2 * cols2), low),
            pltpu.VMEM((owners, rounds, 8, 128), jnp.float32),
            pltpu.VMEM((owners, rounds, 8, 128), jnp.float32),
            pltpu.VMEM((rounds, owners, 8, 128), jnp.float32),
            pltpu.VMEM((rounds, owners, 8, 128), jnp.float32),
            pltpu.VMEM((2 * cols1, 2 * cols1), low),
            pltpu.VMEM((2 * cols1, 2 * cols1), low),
            pltpu.VMEM((2 * cols2, 2 * cols2), low),
            pltpu.VMEM((2 * cols2, 2 * cols2), low),
            pltpu.VMEM((slots, rows, cols1), jnp.float32),
            pltpu.VMEM((slots, rows, cols1), low),
            pltpu.VMEM((slots, rows, cols2), jnp.float32),
            pltpu.VMEM((slots, rows, cols2), low),
        ] + [dma((rounds,))] * 6 + [dma((2,))] + [dma((rounds,))] * 4 + [dma((slots,))] * 4 + [dma((2,))],
        compiler_params=pltpu.CompilerParams(collective_id=0, has_side_effects=True, vmem_limit_bytes=60 * 2 ** 20),
        cost_estimate=pl.CostEstimate(flops=flops, bytes_accessed=10 * (m1.size + m2.size), transcendentals=0),
        name='exchange',
    )(m1, g1, m2, g2)


STEP = 4


def call_plain(kernel, name, steps, in_specs, out_specs, out_shape, args, aliases, traffic):
    return pl.pallas_call(
        kernel, grid=(steps,), in_specs=in_specs, out_specs=out_specs, out_shape=out_shape, input_output_aliases=aliases,
        compiler_params=pltpu.CompilerParams(dimension_semantics=('arbitrary',), vmem_limit_bytes=60 * 2 ** 20),
        cost_estimate=pl.CostEstimate(flops=traffic, bytes_accessed=traffic, transcendentals=0),
        name=name,
    )(*args)


def momentum_kernel(m1_ref, g1_ref, m2_ref, g2_ref, after_ref, new_m1_ref, new_m2_ref):
    new_m1_ref[...] = MOMENTUM * m1_ref[...] + g1_ref[...].astype(jnp.float32)
    new_m2_ref[...] = MOMENTUM * m2_ref[...] + g2_ref[...].astype(jnp.float32)


def momentum_step(m1, g1, m2, g2, after):
    blocks = [pl.BlockSpec((STEP,) + m.shape[1:], lambda i: (i, 0, 0)) for m in (m1, m2)]
    return call_plain(momentum_kernel, 'momentum', m1.shape[0] // STEP,
                      [blocks[0], blocks[0], blocks[1], blocks[1], pl.BlockSpec(memory_space=pl.ANY)], blocks,
                      [jax.ShapeDtypeStruct(m.shape, jnp.float32) for m in (m1, m2)],
                      (m1, g1, m2, g2, after), {}, 10 * (m1.size + m2.size))


def weight_kernel(scales, w1_ref, w2_ref, x1_ref, x2_ref, *refs):
    for scale, w_ref, x_ref, out_ref in zip(scales, (w1_ref, w2_ref), (x1_ref, x2_ref), refs[-2:]):
        w_old = w_ref[...]
        out_ref[...] = w_old - LEARN_RATE * (x_ref[...].astype(jnp.float32) * scale + DECAY * w_old)


def weight_step(w1, w2, x1, x2, scales, first, count, x_columns, into):
    start = first // STEP
    w_specs = [pl.BlockSpec((STEP,) + w.shape[1:], lambda i: (start + i, 0, 0)) for w in (w1, w2)]
    x_specs = [pl.BlockSpec((STEP,) + w.shape[1:], lambda i, c=c: (i, 0, c)) for w, c in zip((w1, w2), x_columns)]
    return call_plain(functools.partial(weight_kernel, scales), 'weights', count // STEP,
                      w_specs + x_specs + [pl.BlockSpec(memory_space=pl.ANY)] * len(into), w_specs,
                      [jax.ShapeDtypeStruct(w.shape, w.dtype) for w in (w1, w2)],
                      (w1, w2, x1, x2, *into), {4 + i: i for i in range(len(into))},
                      10 * count * (w1.size + w2.size) // w1.shape[0])


def solution(mesh):
    data_size = mesh.shape['data']
    model_size = mesh.shape['model']
    owners = data_size * model_size
    block_spec = P('stage', 'data', 'model')

    def local_step(w_fc1, m_fc1, g_fc1, w_fc2, m_fc2, g_fc2):
        experts = w_fc1.shape[0]
        head = experts - owners
        scales = [0.2 * math.sqrt(max(w.shape[1] * data_size, w.shape[2] * model_size)) for w in (w_fc1, w_fc2)]
        back1, back2, last = exchange(m_fc1, g_fc1, m_fc2, g_fc2, owners)
        last = lax.all_to_all(last, ('model', 'data'), 0, 0, tiled=True)
        new_m1, new_m2 = momentum_step(m_fc1, g_fc1, m_fc2, g_fc2, back1)
        part = weight_step(w_fc1, w_fc2, back1, back2, scales, 0, head, (0, 0), ())
        tail_column = w_fc1.shape[2] // w_fc2.shape[2]
        new_w1, new_w2 = weight_step(w_fc1, w_fc2, last, last, scales, head, owners, (0, tail_column), part)
        return new_w1, new_m1, new_w2, new_m2

    return jax.shard_map(local_step, mesh=mesh, in_specs=(block_spec,) * 6, out_specs=(block_spec,) * 4, check_vma=False)
```

```python
import functools
import math
import jax
import jax.numpy as jnp
from jax import lax
from jax.experimental import pallas as pl
from jax.experimental.pallas import tpu as pltpu
from jax.sharding import PartitionSpec as P

NS_STEPS = 5
NS_COEF_A = 3.4445
NS_COEF_B = -4.7750
NS_COEF_C = 2.0315
MOMENTUM = 0.95
LEARN_RATE = 0.04
DECAY = 0.2
NORM_EPS = 1e-7

MESH_ID = pl.DeviceIdType.MESH
GRAM_BLOCK = 256
ROW_BLOCK = 512


def iterate(x_ref, gram_ref, poly_ref):
    rows, cols = x_ref.shape
    gram_block = min(GRAM_BLOCK, cols)
    row_block = min(ROW_BLOCK, rows)

    @pl.loop(0, NS_STEPS)
    def ns_step(_):
        @pl.loop(0, cols // gram_block)
        def gram(i):
            span = pl.ds(pl.multiple_of(i * gram_block, gram_block), gram_block)
            part = lax.dot_general(x_ref[:, span], x_ref[...], (((0,), (0,)), ((), ())), preferred_element_type=jnp.float32)
            gram_ref[span, :] = part.astype(jnp.bfloat16)

        @pl.loop(0, cols // gram_block)
        def poly(i):
            span = pl.ds(pl.multiple_of(i * gram_block, gram_block), gram_block)
            gram_rows = gram_ref[span, :]
            gram_sq = jnp.dot(gram_rows, gram_ref[...], preferred_element_type=jnp.float32)
            poly_ref[span, :] = (NS_COEF_B * gram_rows.astype(jnp.float32) + NS_COEF_C * gram_sq).astype(jnp.bfloat16)

        @pl.loop(0, rows // row_block)
        def update(i):
            span = pl.ds(pl.multiple_of(i * row_block, row_block), row_block)
            x_rows = x_ref[span, :]
            term = jnp.dot(x_rows, poly_ref[...], preferred_element_type=jnp.float32)
            x_ref[span, :] = (NS_COEF_A * x_rows.astype(jnp.float32) + term).astype(jnp.bfloat16)


def momentum_block(m_ref, g_ref, slot, low_ref, index, sq_ref, owner, k):
    new_mom = MOMENTUM * m_ref[slot] + g_ref[slot].astype(jnp.float32)
    m_ref[slot] = new_mom
    low_ref[index] = new_mom.astype(jnp.bfloat16)
    squares = new_mom * new_mom
    rows, cols = squares.shape
    part = jnp.sum(squares.reshape(rows // 8, 8, cols), axis=0)
    total = part[:, :128]
    for start in range(128, cols, 128):
        total = total + part[:, start:start + 128]
    sq_ref[owner, k] = total


AHEAD = 3


def exchange_kernel(m1, g1, m2, g2, new_m1, new_m2, back1, back2, late, low1, low2, x1, x2, sq1, sq2, sums1, sums2,
                    gram1, poly1, gram2, poly2, m_buf1, g_buf1, m_buf2, g_buf2,
                    fwd1, fwd2, got1, got2, ret1, ret2, done_sems, sq_send1, sq_send2, sq_got1, sq_got2,
                    m_sem1, g_sem1, m_sem2, g_sem2, out_sem1, out_sem2, late_sem):
    model = lax.axis_index('model')
    data = lax.axis_index('data')
    chip, core = data // 2, data % 2
    me = model * 4 + data
    owners = 8
    experts = m1.shape[0]
    rounds = experts // owners
    slots = m_buf1.shape[0]
    early1, early2 = back1.shape[0] // owners, back2.shape[0] // owners

    def peer(turn):
        code = owners - 1 - turn
        return (model + code // 4) % 2, ((chip + code // 2 % 2) % 2) * 2 + (core + code % 2) % 2

    def at(place):
        return dict(device_id=(0, place[0], place[1]), device_id_type=MESH_ID)

    def expert(step):
        peer_model, peer_data = peer(step % owners)
        return step // owners * owners + peer_model * 4 + peer_data

    stack1 = (m1, g1, m_buf1, g_buf1, m_sem1, g_sem1)
    stack2 = (m2, g2, m_buf2, g_buf2, m_sem2, g_sem2)

    def loads(stack, step):
        m, g, m_buf, g_buf, m_sem, g_sem = stack
        slot, index = step % slots, expert(step)
        return (pltpu.make_async_copy(m.at[index], m_buf.at[slot], m_sem.at[slot]),
                pltpu.make_async_copy(g.at[index], g_buf.at[slot], g_sem.at[slot]))

    def store(stack, new_m, out_sem, step):
        slot = step % slots
        return pltpu.make_async_copy(stack[2].at[slot], new_m.at[expert(step)], out_sem.at[slot])

    for stack in (stack2, stack1):
        for step in range(AHEAD):
            for load in loads(stack, step):
                load.start()

    barrier = pltpu.get_barrier_semaphore()
    for turn in range(owners - 1):
        pl.semaphore_signal(barrier, inc=1, **at(peer(turn)))
    pl.semaphore_wait(barrier, owners - 1)

    def window(x_ref, k, at_model, at_data):
        rows, cols = x_ref.shape[1] // 4, x_ref.shape[2] // 2
        return x_ref.at[k, pl.ds(pl.multiple_of(at_data * rows, rows), rows), pl.ds(pl.multiple_of(at_model * cols, cols), cols)]

    def forward_round(k, stack, new_m, out_sem, low_ref, x_ref, fwd, got, sq_ref, sums_ref, sq_send, sq_got):
        def send(turn):
            place = peer(turn)
            owner = place[0] * 4 + place[1]
            pltpu.make_async_remote_copy(sq_ref.at[owner, k], sums_ref.at[k, me], sq_send.at[k], sq_got.at[k], **at(place)).start()
            pltpu.make_async_remote_copy(low_ref.at[k * owners + owner], window(x_ref, k, model, data), fwd.at[k], got.at[k],
                                         **at(place)).start()

        @pl.loop(0, owners)
        def block(turn):
            step = k * owners + turn
            index = expert(step)
            for load in loads(stack, step):
                load.wait()
            momentum_block(stack[2], stack[3], step % slots, low_ref, index, sq_ref, index - k * owners, k)
            store(stack, new_m, out_sem, step).start()

            @pl.when(turn > 0)
            def send_before():
                send(turn - 1)

            @pl.when(step >= slots - AHEAD)
            def stored():
                store(stack, new_m, out_sem, step + AHEAD - slots).wait()

            @pl.when(step + AHEAD < experts)
            def prefetch():
                for load in loads(stack, step + AHEAD):
                    load.start()

        pltpu.make_async_copy(sq_ref.at[me, k], sums_ref.at[k, me], sq_got.at[k]).start()
        pltpu.make_async_copy(low_ref.at[k * owners + me], window(x_ref, k, model, data), got.at[k]).start()

    def return_round(k, x_ref, dst, sems, t):
        for turn in range(owners - 1):
            place = peer(turn)
            pltpu.make_async_remote_copy(window(x_ref, k, *place), dst.at[k * owners + me], sems.at[k], done_sems.at[t],
                                         **at(place)).start()
        pltpu.make_async_copy(window(x_ref, k, model, data), dst.at[k * owners + me], done_sems.at[t]).start()

    def keep_round(k, x_ref, columns, sem):
        for holder in range(owners):
            pltpu.make_async_copy(window(x_ref, k, holder // 4, holder % 4), late.at[holder, :, columns], sem).start()

    def wait_bytes(ref, sem):
        pltpu.make_async_copy(ref, ref, sem).wait()

    def orthogonalize(k, x_ref, got, sums_ref, sq_got, gram_ref, poly_ref):
        wait_bytes(sums_ref.at[k], sq_got.at[k])
        wait_bytes(x_ref.at[k], got.at[k])
        norm = jnp.sqrt(jnp.sum(sums_ref[k])) + NORM_EPS
        rows = x_ref.shape[1]

        @pl.loop(0, rows // 256)
        def normalize(i):
            span = pl.ds(pl.multiple_of(i * 256, 256), 256)
            x_ref[k, span, :] = (x_ref[k, span, :].astype(jnp.float32) / norm).astype(jnp.bfloat16)

        iterate(x_ref.at[k], gram_ref, poly_ref)

    @pl.loop(0, rounds)
    def forward(k):
        forward_round(k, stack2, new_m2, out_sem2, low2, x2, fwd2, got2, sq2, sums2, sq_send2, sq_got2)
        forward_round(k, stack1, new_m1, out_sem1, low1, x1, fwd1, got1, sq1, sums1, sq_send1, sq_got1)

    cols1, cols2 = low1.shape[2], low2.shape[2]
    part1, part2 = pl.ds(0, cols1), pl.ds(cols1, cols2)

    @pl.loop(0, rounds)
    def work(k):
        orthogonalize(k, x2, got2, sums2, sq_got2, gram2, poly2)

        @pl.when(k < early2)
        def return2():
            return_round(k, x2, back2, ret2, 0)

        @pl.when(k == early2)
        def keep2():
            keep_round(k, x2, part2, late_sem.at[0])

        orthogonalize(k, x1, got1, sums1, sq_got1, gram1, poly1)

        @pl.when(k < early1)
        def return1():
            return_round(k, x1, back1, ret1, 1)

        @pl.when(k == early1)
        def keep1():
            keep_round(k, x1, part1, late_sem.at[1])

    count = owners - 1
    for stack, new_m, out_sem in ((stack2, new_m2, out_sem2), (stack1, new_m1, out_sem1)):
        for step in range(experts + AHEAD - slots, experts):
            store(stack, new_m, out_sem, step).wait()

    @pl.loop(0, rounds)
    def finish(k):
        for low, sq, fwd, ret, sq_send, early in ((low2, sq2, fwd2, ret2, sq_send2, early2), (low1, sq1, fwd1, ret1, sq_send1, early1)):
            wait_bytes(sq.at[pl.ds(0, count), 0], sq_send.at[k])
            wait_bytes(low.at[pl.ds(0, count)], fwd.at[k])

            @pl.when(k < early)
            def returned():
                wait_bytes(low.at[pl.ds(0, count)], ret.at[k])

    wait_bytes(back2, done_sems.at[0])
    wait_bytes(back1, done_sems.at[1])
    wait_bytes(late.at[:, :, part2], late_sem.at[0])
    wait_bytes(late.at[:, :, part1], late_sem.at[1])


def exchange(m1, g1, m2, g2, owners):
    experts, rows, cols1 = m1.shape
    cols2 = m2.shape[2]
    rounds = experts // owners
    slots = 2 * AHEAD
    any_spec = pl.BlockSpec(memory_space=pl.ANY)
    flops = 2 * rounds * NS_STEPS * sum(2 * 4 * rows * c * c + c ** 3 for c in (2 * cols1, 2 * cols2))
    low = jnp.bfloat16
    dma = pltpu.SemaphoreType.DMA
    results = [((experts, rows, cols1), jnp.float32), ((experts, rows, cols2), jnp.float32),
               ((experts - owners, rows, cols1), low), ((experts - owners, rows, cols2), low),
               ((owners, rows, cols1 + cols2), low)]
    return pl.pallas_call(
        exchange_kernel,
        in_specs=[any_spec] * 4,
        out_specs=[any_spec] * len(results),
        out_shape=[jax.ShapeDtypeStruct(*result) for result in results],
        scratch_shapes=[
            pltpu.VMEM((experts, rows, cols1), low),
            pltpu.VMEM((experts, rows, cols2), low),
            pltpu.VMEM((rounds, 4 * rows, 2 * cols1), low),
            pltpu.VMEM((rounds, 4 * rows, 2 * cols2), low),
            pltpu.VMEM((owners, rounds, 8, 128), jnp.float32),
            pltpu.VMEM((owners, rounds, 8, 128), jnp.float32),
            pltpu.VMEM((rounds, owners, 8, 128), jnp.float32),
            pltpu.VMEM((rounds, owners, 8, 128), jnp.float32),
            pltpu.VMEM((2 * cols1, 2 * cols1), low),
            pltpu.VMEM((2 * cols1, 2 * cols1), low),
            pltpu.VMEM((2 * cols2, 2 * cols2), low),
            pltpu.VMEM((2 * cols2, 2 * cols2), low),
            pltpu.VMEM((slots, rows, cols1), jnp.float32),
            pltpu.VMEM((slots, rows, cols1), low),
            pltpu.VMEM((slots, rows, cols2), jnp.float32),
            pltpu.VMEM((slots, rows, cols2), low),
        ] + [dma((rounds,))] * 6 + [dma((2,))] + [dma((rounds,))] * 4 + [dma((slots,))] * 6 + [dma((2,))],
        compiler_params=pltpu.CompilerParams(collective_id=0, has_side_effects=True, vmem_limit_bytes=62 * 2 ** 20),
        cost_estimate=pl.CostEstimate(flops=flops, bytes_accessed=14 * (m1.size + m2.size), transcendentals=0),
        name='exchange',
    )(m1, g1, m2, g2)


def call_plain(kernel, name, steps, in_specs, out_specs, out_shape, args, aliases, traffic):
    return pl.pallas_call(
        kernel, grid=(steps,), in_specs=in_specs, out_specs=out_specs, out_shape=out_shape, input_output_aliases=aliases,
        compiler_params=pltpu.CompilerParams(dimension_semantics=('arbitrary',), vmem_limit_bytes=60 * 2 ** 20),
        cost_estimate=pl.CostEstimate(flops=traffic, bytes_accessed=traffic, transcendentals=0),
        name=name,
    )(*args)


def weight_block(w_ref, x_ref, out_ref, scale):
    w_old = w_ref[...]
    out_ref[...] = w_old - LEARN_RATE * (x_ref[...].astype(jnp.float32) * scale + DECAY * w_old)


def early_kernel(scales, m1_ref, m2_ref, w1_ref, w2_ref, x1_ref, x2_ref, new_m1_ref, new_m2_ref, new_w1_ref, new_w2_ref):
    new_m1_ref[...] = m1_ref[...]
    new_m2_ref[...] = m2_ref[...]
    weight_block(w1_ref, x1_ref, new_w1_ref, scales[0])
    weight_block(w2_ref, x2_ref, new_w2_ref, scales[1])


def early_step(m1, m2, w1, w2, x1, x2, scales):
    experts, rows = m1.shape[:2]
    back = x1.shape[0]
    steps = 2 * (experts - back)

    def halves(array, count):
        return pl.BlockSpec((count * 2 // steps, rows // 2, array.shape[2]), lambda i: (i // 2, i % 2, 0))

    m_specs = [halves(m, experts) for m in (m1, m2)]
    w_specs = [halves(w, back) for w in (w1, w2)]
    outs = [jax.ShapeDtypeStruct(array.shape, array.dtype) for array in (m1, m2, w1, w2)]
    traffic = 8 * (m1.size + m2.size) + 10 * (x1.size + x2.size)
    return call_plain(functools.partial(early_kernel, scales), 'early', steps, m_specs + w_specs + w_specs, m_specs + w_specs,
                      outs, (m1, m2, w1, w2, x1, x2), {}, traffic)


def late_kernel(scales, w1_ref, w2_ref, x1_ref, x2_ref, into1_ref, into2_ref, new_w1_ref, new_w2_ref):
    weight_block(w1_ref, x1_ref, new_w1_ref, scales[0])
    weight_block(w2_ref, x2_ref, new_w2_ref, scales[1])


def late_step(w1, w2, late, into1, into2, scales):
    count = late.shape[0]
    first = w1.shape[0] - count
    column = w1.shape[2] // w2.shape[2]
    w_specs = [pl.BlockSpec((1,) + w.shape[1:], lambda i: (first + i, 0, 0)) for w in (w1, w2)]
    x_specs = [pl.BlockSpec((1,) + w.shape[1:], lambda i, c=c: (i, 0, c)) for w, c in ((w1, 0), (w2, column))]
    return call_plain(functools.partial(late_kernel, scales), 'late', count,
                      w_specs + x_specs + [pl.BlockSpec(memory_space=pl.ANY)] * 2, w_specs,
                      [jax.ShapeDtypeStruct(w.shape, w.dtype) for w in (w1, w2)],
                      (w1, w2, late, late, into1, into2), {4: 0, 5: 1}, 10 * late.size)


def solution(mesh):
    data_size = mesh.shape['data']
    model_size = mesh.shape['model']
    owners = data_size * model_size
    block_spec = P('stage', 'data', 'model')

    def local_step(w_fc1, m_fc1, g_fc1, w_fc2, m_fc2, g_fc2):
        scales = [0.2 * math.sqrt(max(w.shape[1] * data_size, w.shape[2] * model_size)) for w in (w_fc1, w_fc2)]
        new_m1, new_m2, back1, back2, late = exchange(m_fc1, g_fc1, m_fc2, g_fc2, owners)
        late = lax.all_to_all(late, ('model', 'data'), 0, 0, tiled=True)
        new_m1, new_m2, new_w1, new_w2 = early_step(new_m1, new_m2, w_fc1, w_fc2, back1, back2, scales)
        new_w1, new_w2 = late_step(w_fc1, w_fc2, late, new_w1, new_w2, scales)
        return new_w1, new_m1, new_w2, new_m2

    return jax.shard_map(local_step, mesh=mesh, in_specs=(block_spec,) * 6, out_specs=(block_spec,) * 4, check_vma=False)
```

```python
import functools
import math
import jax
import jax.numpy as jnp
from jax import lax
from jax.experimental import pallas as pl
from jax.experimental.pallas import tpu as pltpu
from jax.sharding import PartitionSpec as P

NS_STEPS = 5
NS_COEF_A = 3.4445
NS_COEF_B = -4.7750
NS_COEF_C = 2.0315
MOMENTUM = 0.95
LEARN_RATE = 0.04
DECAY = 0.2
NORM_EPS = 1e-7

MESH_ID = pl.DeviceIdType.MESH
GRAM_BLOCK = 256
ROW_BLOCK = 512


def iterate(x_ref, gram_ref, poly_ref):
    rows, cols = x_ref.shape
    gram_block = min(GRAM_BLOCK, cols)
    row_block = min(ROW_BLOCK, rows)

    @pl.loop(0, NS_STEPS)
    def ns_step(_):
        @pl.loop(0, cols // gram_block)
        def gram(i):
            span = pl.ds(pl.multiple_of(i * gram_block, gram_block), gram_block)
            part = lax.dot_general(x_ref[:, span], x_ref[...], (((0,), (0,)), ((), ())), preferred_element_type=jnp.float32)
            gram_ref[span, :] = part.astype(jnp.bfloat16)

        @pl.loop(0, cols // gram_block)
        def poly(i):
            span = pl.ds(pl.multiple_of(i * gram_block, gram_block), gram_block)
            gram_rows = gram_ref[span, :]
            gram_sq = jnp.dot(gram_rows, gram_ref[...], preferred_element_type=jnp.float32)
            poly_ref[span, :] = (NS_COEF_B * gram_rows.astype(jnp.float32) + NS_COEF_C * gram_sq).astype(jnp.bfloat16)

        @pl.loop(0, rows // row_block)
        def update(i):
            span = pl.ds(pl.multiple_of(i * row_block, row_block), row_block)
            x_rows = x_ref[span, :]
            term = jnp.dot(x_rows, poly_ref[...], preferred_element_type=jnp.float32)
            x_ref[span, :] = (NS_COEF_A * x_rows.astype(jnp.float32) + term).astype(jnp.bfloat16)


def momentum_block(m_ref, g_ref, slot, low_ref, index, sq_ref, owner, k):
    new_mom = MOMENTUM * m_ref[slot] + g_ref[slot].astype(jnp.float32)
    m_ref[slot] = new_mom
    low_ref[index] = new_mom.astype(jnp.bfloat16)
    squares = new_mom * new_mom
    rows, cols = squares.shape
    part = jnp.sum(squares.reshape(rows // 8, 8, cols), axis=0)
    total = part[:, :128]
    for start in range(128, cols, 128):
        total = total + part[:, start:start + 128]
    sq_ref[owner, k] = total


AHEAD = 3
LATE = 2
DIAGONAL = 2


def exchange_kernel(m1, g1, m2, g2, new_m1, new_m2, back1, back2, late_a, late_b, low1, low2, x1, x2, sq1, sq2, sums1, sums2,
                    gram1, poly1, gram2, poly2, m_buf1, g_buf1, m_buf2, g_buf2,
                    fwd1, fwd2, got1, got2, ret1, ret2, done_sems, sq_send1, sq_send2, sq_got1, sq_got2,
                    m_sem1, g_sem1, m_sem2, g_sem2, out_sem1, out_sem2, late_sem):
    model = lax.axis_index('model')
    data = lax.axis_index('data')
    chip, core = data // 2, data % 2
    me = model * 4 + data
    owners = 8
    experts = m1.shape[0]
    rounds = experts // owners
    slots = m_buf1.shape[0]
    early = rounds - LATE

    def peer(turn):
        code = owners - 1 - turn
        return (model + code // 4) % 2, ((chip + code // 2 % 2) % 2) * 2 + (core + code % 2) % 2

    def at(place):
        return dict(device_id=(0, place[0], place[1]), device_id_type=MESH_ID)

    def expert(step):
        peer_model, peer_data = peer(step % owners)
        return step // owners * owners + peer_model * 4 + peer_data

    stack1 = (m1, g1, m_buf1, g_buf1, m_sem1, g_sem1)
    stack2 = (m2, g2, m_buf2, g_buf2, m_sem2, g_sem2)

    def loads(stack, step):
        m, g, m_buf, g_buf, m_sem, g_sem = stack
        slot, index = step % slots, expert(step)
        return (pltpu.make_async_copy(m.at[index], m_buf.at[slot], m_sem.at[slot]),
                pltpu.make_async_copy(g.at[index], g_buf.at[slot], g_sem.at[slot]))

    def store(stack, new_m, out_sem, step):
        slot = step % slots
        return pltpu.make_async_copy(stack[2].at[slot], new_m.at[expert(step)], out_sem.at[slot])

    for stack in (stack2, stack1):
        for step in range(AHEAD):
            for load in loads(stack, step):
                load.start()

    barrier = pltpu.get_barrier_semaphore()
    for turn in range(owners - 1):
        pl.semaphore_signal(barrier, inc=1, **at(peer(turn)))
    pl.semaphore_wait(barrier, owners - 1)

    def window(x_ref, k, at_model, at_data):
        rows, cols = x_ref.shape[1] // 4, x_ref.shape[2] // 2
        return x_ref.at[k, pl.ds(pl.multiple_of(at_data * rows, rows), rows), pl.ds(pl.multiple_of(at_model * cols, cols), cols)]

    def forward_round(k, stack, new_m, out_sem, low_ref, x_ref, fwd, got, sq_ref, sums_ref, sq_send, sq_got):
        def send(turn):
            place = peer(turn)
            owner = place[0] * 4 + place[1]
            pltpu.make_async_remote_copy(sq_ref.at[owner, k], sums_ref.at[k, me], sq_send.at[k], sq_got.at[k], **at(place)).start()
            pltpu.make_async_remote_copy(low_ref.at[k * owners + owner], window(x_ref, k, model, data), fwd.at[k], got.at[k],
                                         **at(place)).start()

        @pl.loop(0, owners)
        def block(turn):
            step = k * owners + turn
            index = expert(step)
            for load in loads(stack, step):
                load.wait()
            momentum_block(stack[2], stack[3], step % slots, low_ref, index, sq_ref, index - k * owners, k)
            store(stack, new_m, out_sem, step).start()

            @pl.when(turn > 0)
            def send_before():
                send(turn - 1)

            @pl.when(step >= slots - AHEAD)
            def stored():
                store(stack, new_m, out_sem, step + AHEAD - slots).wait()

            @pl.when(step + AHEAD < experts)
            def prefetch():
                for load in loads(stack, step + AHEAD):
                    load.start()

        pltpu.make_async_copy(sq_ref.at[me, k], sums_ref.at[k, me], sq_got.at[k]).start()
        pltpu.make_async_copy(low_ref.at[k * owners + me], window(x_ref, k, model, data), got.at[k]).start()

    def return_round(k, x_ref, dst, sems, t, first_column, late_sems):
        def give(turn):
            place = peer(turn)
            pltpu.make_async_remote_copy(window(x_ref, k, *place), dst.at[k * owners + me], sems.at[k], done_sems.at[t],
                                         **at(place)).start()

        @pl.when(k < early)
        def to_diagonal():
            for turn in range(DIAGONAL):
                give(turn)

        for turn in range(DIAGONAL, owners - 1):
            give(turn)
        pltpu.make_async_copy(window(x_ref, k, model, data), dst.at[k * owners + me], done_sems.at[t]).start()

        @pl.when(k >= early)
        def keep():
            cols = dst.shape[2]
            span = pl.ds(pl.multiple_of(first_column + (k - early) * cols, cols), cols)
            for turn, late in ((1, late_a), (0, late_b)):
                pltpu.make_async_copy(window(x_ref, k, *peer(turn)), late.at[:, span], late_sems.at[turn]).start()

    def wait_bytes(ref, sem):
        pltpu.make_async_copy(ref, ref, sem).wait()

    def orthogonalize(k, x_ref, got, sums_ref, sq_got, gram_ref, poly_ref):
        wait_bytes(sums_ref.at[k], sq_got.at[k])
        wait_bytes(x_ref.at[k], got.at[k])
        norm = jnp.sqrt(jnp.sum(sums_ref[k])) + NORM_EPS
        rows = x_ref.shape[1]

        @pl.loop(0, rows // 256)
        def normalize(i):
            span = pl.ds(pl.multiple_of(i * 256, 256), 256)
            x_ref[k, span, :] = (x_ref[k, span, :].astype(jnp.float32) / norm).astype(jnp.bfloat16)

        iterate(x_ref.at[k], gram_ref, poly_ref)

    @pl.loop(0, rounds)
    def forward(k):
        forward_round(k, stack2, new_m2, out_sem2, low2, x2, fwd2, got2, sq2, sums2, sq_send2, sq_got2)
        forward_round(k, stack1, new_m1, out_sem1, low1, x1, fwd1, got1, sq1, sums1, sq_send1, sq_got1)

    cols1, cols2 = low1.shape[2], low2.shape[2]

    @pl.loop(0, rounds)
    def work(k):
        orthogonalize(k, x2, got2, sums2, sq_got2, gram2, poly2)
        return_round(k, x2, back2, ret2, 0, LATE * cols1, late_sem)
        orthogonalize(k, x1, got1, sums1, sq_got1, gram1, poly1)
        return_round(k, x1, back1, ret1, 1, 0, late_sem)

    count = owners - 1
    for stack, new_m, out_sem in ((stack2, new_m2, out_sem2), (stack1, new_m1, out_sem1)):
        for step in range(experts + AHEAD - slots, experts):
            store(stack, new_m, out_sem, step).wait()

    @pl.loop(0, rounds)
    def finish(k):
        for low, sq, fwd, ret, sq_send in ((low2, sq2, fwd2, ret2, sq_send2), (low1, sq1, fwd1, ret1, sq_send1)):
            wait_bytes(sq.at[pl.ds(0, count), 0], sq_send.at[k])
            wait_bytes(low.at[pl.ds(0, count)], fwd.at[k])

            wait_bytes(low.at[pl.ds(0, count - DIAGONAL)], ret.at[k])

            @pl.when(k < early)
            def returned():
                wait_bytes(low.at[pl.ds(0, DIAGONAL)], ret.at[k])

    here = experts - LATE * DIAGONAL
    wait_bytes(back2.at[pl.ds(0, here)], done_sems.at[0])
    wait_bytes(back1.at[pl.ds(0, here)], done_sems.at[1])
    wait_bytes(late_b, late_sem.at[0])
    wait_bytes(late_a, late_sem.at[1])


def exchange(m1, g1, m2, g2, owners):
    experts, rows, cols1 = m1.shape
    cols2 = m2.shape[2]
    rounds = experts // owners
    slots = 2 * AHEAD
    any_spec = pl.BlockSpec(memory_space=pl.ANY)
    flops = 2 * rounds * NS_STEPS * sum(2 * 4 * rows * c * c + c ** 3 for c in (2 * cols1, 2 * cols2))
    low = jnp.bfloat16
    dma = pltpu.SemaphoreType.DMA
    results = [((experts, rows, cols1), jnp.float32), ((experts, rows, cols2), jnp.float32),
               ((experts, rows, cols1), low), ((experts, rows, cols2), low),
               ((rows, LATE * (cols1 + cols2)), low), ((rows, LATE * (cols1 + cols2)), low)]
    return pl.pallas_call(
        exchange_kernel,
        in_specs=[any_spec] * 4,
        out_specs=[any_spec] * len(results),
        out_shape=[jax.ShapeDtypeStruct(*result) for result in results],
        scratch_shapes=[
            pltpu.VMEM((experts, rows, cols1), low),
            pltpu.VMEM((experts, rows, cols2), low),
            pltpu.VMEM((rounds, 4 * rows, 2 * cols1), low),
            pltpu.VMEM((rounds, 4 * rows, 2 * cols2), low),
            pltpu.VMEM((owners, rounds, 8, 128), jnp.float32),
            pltpu.VMEM((owners, rounds, 8, 128), jnp.float32),
            pltpu.VMEM((rounds, owners, 8, 128), jnp.float32),
            pltpu.VMEM((rounds, owners, 8, 128), jnp.float32),
            pltpu.VMEM((2 * cols1, 2 * cols1), low),
            pltpu.VMEM((2 * cols1, 2 * cols1), low),
            pltpu.VMEM((2 * cols2, 2 * cols2), low),
            pltpu.VMEM((2 * cols2, 2 * cols2), low),
            pltpu.VMEM((slots, rows, cols1), jnp.float32),
            pltpu.VMEM((slots, rows, cols1), low),
            pltpu.VMEM((slots, rows, cols2), jnp.float32),
            pltpu.VMEM((slots, rows, cols2), low),
        ] + [dma((rounds,))] * 6 + [dma((2,))] + [dma((rounds,))] * 4 + [dma((slots,))] * 6 + [dma((2,))],
        compiler_params=pltpu.CompilerParams(collective_id=0, has_side_effects=True, vmem_limit_bytes=62 * 2 ** 20),
        cost_estimate=pl.CostEstimate(flops=flops, bytes_accessed=14 * (m1.size + m2.size), transcendentals=0),
        name='exchange',
    )(m1, g1, m2, g2)


def call_plain(kernel, name, steps, in_specs, out_specs, out_shape, place, args, aliases, traffic):
    return pl.pallas_call(
        kernel,
        grid_spec=pltpu.PrefetchScalarGridSpec(num_scalar_prefetch=1, grid=(steps,), in_specs=in_specs, out_specs=out_specs),
        out_shape=out_shape, input_output_aliases=aliases,
        compiler_params=pltpu.CompilerParams(dimension_semantics=('arbitrary',), vmem_limit_bytes=60 * 2 ** 20),
        cost_estimate=pl.CostEstimate(flops=traffic, bytes_accessed=traffic, transcendentals=0),
        name=name,
    )(place, *args)


def weight_block(w_ref, x_mat, out_ref, scale):
    w_old = w_ref[0]
    out_ref[0] = w_old - LEARN_RATE * (x_mat.astype(jnp.float32) * scale + DECAY * w_old)


def early_kernel(scales, place, m1_ref, m2_ref, w1_ref, w2_ref, x1_ref, x2_ref, new_m1_ref, new_m2_ref, new_w1_ref, new_w2_ref):
    new_m1_ref[...] = m1_ref[...]
    new_m2_ref[...] = m2_ref[...]
    weight_block(w1_ref, x1_ref[0], new_w1_ref, scales[0])
    weight_block(w2_ref, x2_ref[0], new_w2_ref, scales[1])


def early_step(m1, m2, w1, w2, x1, x2, scales, pair, owners):
    experts = m1.shape[0]
    first_late = experts - LATE * owners

    def turn(i, place):
        late = (place[0] * 2 + 2 + jnp.minimum(i % owners, owners - DIAGONAL - 1)) % owners
        return jnp.where(i < first_late, i, i // owners * owners + late), 0, 0

    m_specs = [pl.BlockSpec((1,) + m.shape[1:], lambda i, place: (i, 0, 0)) for m in (m1, m2)]
    w_specs = [pl.BlockSpec((1,) + w.shape[1:], turn) for w in (w1, w2)]
    outs = [jax.ShapeDtypeStruct(array.shape, array.dtype) for array in (m1, m2, w1, w2)]
    traffic = 18 * (m1.size + m2.size)
    return call_plain(functools.partial(early_kernel, scales), 'early', experts, m_specs + w_specs + w_specs, m_specs + w_specs,
                      outs, pair, (m1, m2, w1, w2, x1, x2), {}, traffic)


def late_kernel(scales, place, w1_ref, w2_ref, x1_ref, x2_ref, into1_ref, into2_ref, new_w1_ref, new_w2_ref):
    weight_block(w1_ref, x1_ref[...], new_w1_ref, scales[0])
    weight_block(w2_ref, x2_ref[...], new_w2_ref, scales[1])


def late_step(w1, w2, late, into1, into2, scales, owner, owners):
    first_round = w1.shape[0] // owners - LATE
    column = LATE * w1.shape[2] // w2.shape[2]
    w_specs = [pl.BlockSpec((1,) + w.shape[1:], lambda i, place: ((first_round + i) * owners + place[0], 0, 0)) for w in (w1, w2)]
    x_specs = [pl.BlockSpec(w.shape[1:], lambda i, place, c=c: (0, c + i)) for w, c in ((w1, 0), (w2, column))]
    return call_plain(functools.partial(late_kernel, scales), 'late', LATE,
                      w_specs + x_specs + [pl.BlockSpec(memory_space=pl.ANY)] * 2, w_specs,
                      [jax.ShapeDtypeStruct(w.shape, w.dtype) for w in (w1, w2)],
                      owner, (w1, w2, late, late, into1, into2), {5: 0, 6: 1}, 5 * late.size)


def solution(mesh):
    data_size = mesh.shape['data']
    model_size = mesh.shape['model']
    owners = data_size * model_size
    block_spec = P('stage', 'data', 'model')

    def local_step(w_fc1, m_fc1, g_fc1, w_fc2, m_fc2, g_fc2):
        scales = [0.2 * math.sqrt(max(w.shape[1] * data_size, w.shape[2] * model_size)) for w in (w_fc1, w_fc2)]
        model, data = lax.axis_index('model'), lax.axis_index('data')
        pair = 3 - model * 2 - (data >> 1)
        new_m1, new_m2, back1, back2, late_a, late_b = exchange(m_fc1, g_fc1, m_fc2, g_fc2, owners)
        late_a = lax.ppermute(late_a, ('model', 'data'), [(i, i ^ 6) for i in range(owners)])
        late_b = lax.ppermute(late_b, ('model', 'data'), [(i, i ^ 7) for i in range(owners)])
        new_m1, new_m2, new_w1, new_w2 = early_step(new_m1, new_m2, w_fc1, w_fc2, back1, back2, scales, pair[None], owners)
        same = pair * 2 + (data & 1)
        cross = same ^ 1
        new_w1, new_w2 = late_step(w_fc1, w_fc2, late_a, new_w1, new_w2, scales, same[None], owners)
        new_w1, new_w2 = late_step(w_fc1, w_fc2, late_b, new_w1, new_w2, scales, cross[None], owners)
        return new_w1, new_m1, new_w2, new_m2

    return jax.shard_map(local_step, mesh=mesh, in_specs=(block_spec,) * 6, out_specs=(block_spec,) * 4, check_vma=False)
```

```python
import functools
import math
import jax
import jax.numpy as jnp
from jax import lax
from jax.experimental import pallas as pl
from jax.experimental.pallas import tpu as pltpu
from jax.sharding import PartitionSpec as P

NS_STEPS = 5
NS_COEF_A = 3.4445
NS_COEF_B = -4.7750
NS_COEF_C = 2.0315
MOMENTUM = 0.95
LEARN_RATE = 0.04
DECAY = 0.2
NORM_EPS = 1e-7

MESH_ID = pl.DeviceIdType.MESH
GRAM_BLOCK = 256
ROW_BLOCK = 512


def iterate(x_ref, gram_ref, poly_ref):
    rows, cols = x_ref.shape
    gram_block = min(GRAM_BLOCK, cols)
    row_block = min(ROW_BLOCK, rows)

    @pl.loop(0, NS_STEPS)
    def ns_step(_):
        @pl.loop(0, cols // gram_block)
        def gram(i):
            span = pl.ds(pl.multiple_of(i * gram_block, gram_block), gram_block)
            part = lax.dot_general(x_ref[:, span], x_ref[...], (((0,), (0,)), ((), ())), preferred_element_type=jnp.float32)
            gram_ref[span, :] = part.astype(jnp.bfloat16)

        @pl.loop(0, cols // gram_block)
        def poly(i):
            span = pl.ds(pl.multiple_of(i * gram_block, gram_block), gram_block)
            gram_rows = gram_ref[span, :]
            gram_sq = jnp.dot(gram_rows, gram_ref[...], preferred_element_type=jnp.float32)
            poly_ref[span, :] = (NS_COEF_B * gram_rows.astype(jnp.float32) + NS_COEF_C * gram_sq).astype(jnp.bfloat16)

        @pl.loop(0, rows // row_block)
        def update(i):
            span = pl.ds(pl.multiple_of(i * row_block, row_block), row_block)
            x_rows = x_ref[span, :]
            term = jnp.dot(x_rows, poly_ref[...], preferred_element_type=jnp.float32)
            x_ref[span, :] = (NS_COEF_A * x_rows.astype(jnp.float32) + term).astype(jnp.bfloat16)


def momentum_block(m_ref, g_ref, slot, low_ref, index, sq_ref, owner, k):
    new_mom = MOMENTUM * m_ref[slot] + g_ref[slot].astype(jnp.float32)
    m_ref[slot] = new_mom
    low_ref[index] = new_mom.astype(jnp.bfloat16)
    squares = new_mom * new_mom
    rows, cols = squares.shape
    part = jnp.sum(squares.reshape(rows // 8, 8, cols), axis=0)
    total = part[:, :128]
    for start in range(128, cols, 128):
        total = total + part[:, start:start + 128]
    sq_ref[owner, k] = total


AHEAD = 3
LATE = (2, 3)
DIAGONAL = 2


def exchange_kernel(m1, g1, m2, g2, new_m1, new_m2, back1, back2, late_a, late_b, low1, low2, x1, x2, sq1, sq2, sums1, sums2,
                    gram1, poly1, gram2, poly2, m_buf1, g_buf1, m_buf2, g_buf2,
                    fwd1, fwd2, got1, got2, ret1, ret2, done_sems, sq_send1, sq_send2, sq_got1, sq_got2,
                    m_sem1, g_sem1, m_sem2, g_sem2, out_sem1, out_sem2, late_sem):
    model = lax.axis_index('model')
    data = lax.axis_index('data')
    chip, core = data // 2, data % 2
    me = model * 4 + data
    owners = 8
    experts = m1.shape[0]
    rounds = experts // owners
    slots = m_buf1.shape[0]
    early1, early2 = (rounds - late for late in LATE)

    def peer(turn):
        code = owners - 1 - turn
        return (model + code // 4) % 2, ((chip + code // 2 % 2) % 2) * 2 + (core + code % 2) % 2

    def at(place):
        return dict(device_id=(0, place[0], place[1]), device_id_type=MESH_ID)

    def expert(step):
        peer_model, peer_data = peer(step % owners)
        return step // owners * owners + peer_model * 4 + peer_data

    stack1 = (m1, g1, m_buf1, g_buf1, m_sem1, g_sem1)
    stack2 = (m2, g2, m_buf2, g_buf2, m_sem2, g_sem2)

    def loads(stack, step):
        m, g, m_buf, g_buf, m_sem, g_sem = stack
        slot, index = step % slots, expert(step)
        return (pltpu.make_async_copy(m.at[index], m_buf.at[slot], m_sem.at[slot]),
                pltpu.make_async_copy(g.at[index], g_buf.at[slot], g_sem.at[slot]))

    def store(stack, new_m, out_sem, step):
        slot = step % slots
        return pltpu.make_async_copy(stack[2].at[slot], new_m.at[expert(step)], out_sem.at[slot])

    for stack in (stack2, stack1):
        for step in range(AHEAD):
            for load in loads(stack, step):
                load.start()

    barrier = pltpu.get_barrier_semaphore()
    for turn in range(owners - 1):
        pl.semaphore_signal(barrier, inc=1, **at(peer(turn)))
    pl.semaphore_wait(barrier, owners - 1)

    def window(x_ref, k, at_model, at_data):
        rows, cols = x_ref.shape[1] // 4, x_ref.shape[2] // 2
        return x_ref.at[k, pl.ds(pl.multiple_of(at_data * rows, rows), rows), pl.ds(pl.multiple_of(at_model * cols, cols), cols)]

    def forward_round(k, stack, new_m, out_sem, low_ref, x_ref, fwd, got, sq_ref, sums_ref, sq_send, sq_got):
        def send(turn):
            place = peer(turn)
            owner = place[0] * 4 + place[1]
            pltpu.make_async_remote_copy(sq_ref.at[owner, k], sums_ref.at[k, me], sq_send.at[k], sq_got.at[k], **at(place)).start()
            pltpu.make_async_remote_copy(low_ref.at[k * owners + owner], window(x_ref, k, model, data), fwd.at[k], got.at[k],
                                         **at(place)).start()

        @pl.loop(0, owners)
        def block(turn):
            step = k * owners + turn
            index = expert(step)
            for load in loads(stack, step):
                load.wait()
            momentum_block(stack[2], stack[3], step % slots, low_ref, index, sq_ref, index - k * owners, k)
            store(stack, new_m, out_sem, step).start()

            @pl.when(turn > 0)
            def send_before():
                send(turn - 1)

            @pl.when(step >= slots - AHEAD)
            def stored():
                store(stack, new_m, out_sem, step + AHEAD - slots).wait()

            @pl.when(step + AHEAD < experts)
            def prefetch():
                for load in loads(stack, step + AHEAD):
                    load.start()

        pltpu.make_async_copy(sq_ref.at[me, k], sums_ref.at[k, me], sq_got.at[k]).start()
        pltpu.make_async_copy(low_ref.at[k * owners + me], window(x_ref, k, model, data), got.at[k]).start()

    def return_round(k, x_ref, dst, sems, t, early, first_column):
        def give(turn):
            place = peer(turn)
            pltpu.make_async_remote_copy(window(x_ref, k, *place), dst.at[k * owners + me], sems.at[k], done_sems.at[t],
                                         **at(place)).start()

        @pl.when(k < early)
        def to_diagonal():
            for turn in range(DIAGONAL):
                give(turn)

        for turn in range(DIAGONAL, owners - 1):
            give(turn)
        pltpu.make_async_copy(window(x_ref, k, model, data), dst.at[k * owners + me], done_sems.at[t]).start()

        @pl.when(k >= early)
        def keep():
            cols = dst.shape[2]
            span = pl.ds(pl.multiple_of(first_column + (k - early) * cols, cols), cols)
            for turn, late in ((1, late_a), (0, late_b)):
                pltpu.make_async_copy(window(x_ref, k, *peer(turn)), late.at[:, span], late_sem.at[turn]).start()

    def wait_bytes(ref, sem):
        pltpu.make_async_copy(ref, ref, sem).wait()

    def orthogonalize(k, x_ref, got, sums_ref, sq_got, gram_ref, poly_ref):
        wait_bytes(sums_ref.at[k], sq_got.at[k])
        wait_bytes(x_ref.at[k], got.at[k])
        norm = jnp.sqrt(jnp.sum(sums_ref[k])) + NORM_EPS
        rows = x_ref.shape[1]

        @pl.loop(0, rows // 256)
        def normalize(i):
            span = pl.ds(pl.multiple_of(i * 256, 256), 256)
            x_ref[k, span, :] = (x_ref[k, span, :].astype(jnp.float32) / norm).astype(jnp.bfloat16)

        iterate(x_ref.at[k], gram_ref, poly_ref)

    @pl.loop(0, rounds)
    def forward(k):
        forward_round(k, stack2, new_m2, out_sem2, low2, x2, fwd2, got2, sq2, sums2, sq_send2, sq_got2)
        forward_round(k, stack1, new_m1, out_sem1, low1, x1, fwd1, got1, sq1, sums1, sq_send1, sq_got1)

    cols1, cols2 = low1.shape[2], low2.shape[2]

    @pl.loop(0, rounds)
    def work(k):
        orthogonalize(k, x2, got2, sums2, sq_got2, gram2, poly2)
        return_round(k, x2, back2, ret2, 0, early2, LATE[0] * cols1)
        orthogonalize(k, x1, got1, sums1, sq_got1, gram1, poly1)
        return_round(k, x1, back1, ret1, 1, early1, 0)

    count = owners - 1
    for stack, new_m, out_sem in ((stack2, new_m2, out_sem2), (stack1, new_m1, out_sem1)):
        for step in range(experts + AHEAD - slots, experts):
            store(stack, new_m, out_sem, step).wait()

    @pl.loop(0, rounds)
    def finish(k):
        for low, sq, fwd, ret, sq_send, early in ((low2, sq2, fwd2, ret2, sq_send2, early2), (low1, sq1, fwd1, ret1, sq_send1, early1)):
            wait_bytes(sq.at[pl.ds(0, count), 0], sq_send.at[k])
            wait_bytes(low.at[pl.ds(0, count)], fwd.at[k])

            wait_bytes(low.at[pl.ds(0, count - DIAGONAL)], ret.at[k])

            @pl.when(k < early)
            def returned():
                wait_bytes(low.at[pl.ds(0, DIAGONAL)], ret.at[k])

    wait_bytes(back2.at[pl.ds(0, experts - LATE[1] * DIAGONAL)], done_sems.at[0])
    wait_bytes(back1.at[pl.ds(0, experts - LATE[0] * DIAGONAL)], done_sems.at[1])
    wait_bytes(late_b, late_sem.at[0])
    wait_bytes(late_a, late_sem.at[1])


def exchange(m1, g1, m2, g2, owners):
    experts, rows, cols1 = m1.shape
    cols2 = m2.shape[2]
    rounds = experts // owners
    slots = 2 * AHEAD
    any_spec = pl.BlockSpec(memory_space=pl.ANY)
    flops = 2 * rounds * NS_STEPS * sum(2 * 4 * rows * c * c + c ** 3 for c in (2 * cols1, 2 * cols2))
    low = jnp.bfloat16
    dma = pltpu.SemaphoreType.DMA
    results = [((experts, rows, cols1), jnp.float32), ((experts, rows, cols2), jnp.float32),
               ((experts, rows, cols1), low), ((experts, rows, cols2), low),
               ((rows, LATE[0] * cols1 + LATE[1] * cols2), low), ((rows, LATE[0] * cols1 + LATE[1] * cols2), low)]
    return pl.pallas_call(
        exchange_kernel,
        in_specs=[any_spec] * 4,
        out_specs=[any_spec] * len(results),
        out_shape=[jax.ShapeDtypeStruct(*result) for result in results],
        scratch_shapes=[
            pltpu.VMEM((experts, rows, cols1), low),
            pltpu.VMEM((experts, rows, cols2), low),
            pltpu.VMEM((rounds, 4 * rows, 2 * cols1), low),
            pltpu.VMEM((rounds, 4 * rows, 2 * cols2), low),
            pltpu.VMEM((owners, rounds, 8, 128), jnp.float32),
            pltpu.VMEM((owners, rounds, 8, 128), jnp.float32),
            pltpu.VMEM((rounds, owners, 8, 128), jnp.float32),
            pltpu.VMEM((rounds, owners, 8, 128), jnp.float32),
            pltpu.VMEM((2 * cols1, 2 * cols1), low),
            pltpu.VMEM((2 * cols1, 2 * cols1), low),
            pltpu.VMEM((2 * cols2, 2 * cols2), low),
            pltpu.VMEM((2 * cols2, 2 * cols2), low),
            pltpu.VMEM((slots, rows, cols1), jnp.float32),
            pltpu.VMEM((slots, rows, cols1), low),
            pltpu.VMEM((slots, rows, cols2), jnp.float32),
            pltpu.VMEM((slots, rows, cols2), low),
        ] + [dma((rounds,))] * 6 + [dma((2,))] + [dma((rounds,))] * 4 + [dma((slots,))] * 6 + [dma((2,))],
        compiler_params=pltpu.CompilerParams(collective_id=0, has_side_effects=True, vmem_limit_bytes=62 * 2 ** 20),
        cost_estimate=pl.CostEstimate(flops=flops, bytes_accessed=14 * (m1.size + m2.size), transcendentals=0),
        name='exchange',
    )(m1, g1, m2, g2)


def call_plain(kernel, name, steps, in_specs, out_specs, out_shape, place, args, aliases, traffic, limit):
    return pl.pallas_call(
        kernel,
        grid_spec=pltpu.PrefetchScalarGridSpec(num_scalar_prefetch=1, grid=(steps,), in_specs=in_specs, out_specs=out_specs),
        out_shape=out_shape, input_output_aliases=aliases,
        compiler_params=pltpu.CompilerParams(dimension_semantics=('arbitrary',), vmem_limit_bytes=limit * 2 ** 20),
        cost_estimate=pl.CostEstimate(flops=traffic, bytes_accessed=traffic, transcendentals=0),
        name=name,
    )(place, *args)


def weight_block(w_ref, x_mat, out_ref, scale):
    w_old = w_ref[...]
    out_ref[...] = w_old - LEARN_RATE * (x_mat.astype(jnp.float32) * scale + DECAY * w_old)


def early_kernel(scales, place, m1_ref, m2_ref, w1_ref, w2_ref, x1_ref, x2_ref, new_m1_ref, new_m2_ref, new_w1_ref, new_w2_ref):
    new_m1_ref[...] = m1_ref[...]
    new_m2_ref[...] = m2_ref[...]
    weight_block(w1_ref, x1_ref[...], new_w1_ref, scales[0])
    weight_block(w2_ref, x2_ref[...], new_w2_ref, scales[1])


def early_step(m1, m2, w1, w2, x1, x2, scales, pair, owners):
    steps, pairs = m1.shape[0] // 2, owners // 2

    def spec(array, late):
        def turn(i, place):
            other = (place[0] + 1 + jnp.minimum(i % pairs, pairs - 2)) % pairs
            return jnp.where(i < steps - late * pairs, i, i // pairs * pairs + other), 0, 0

        return pl.BlockSpec((2,) + array.shape[1:], turn)

    m_specs = [pl.BlockSpec((2,) + m.shape[1:], lambda i, place: (i, 0, 0)) for m in (m1, m2)]
    w_specs = [spec(w, late) for w, late in zip((w1, w2), LATE)]
    outs = [jax.ShapeDtypeStruct(array.shape, array.dtype) for array in (m1, m2, w1, w2)]
    traffic = 18 * (m1.size + m2.size)
    return call_plain(functools.partial(early_kernel, scales), 'early', steps, m_specs + w_specs + w_specs, m_specs + w_specs,
                      outs, pair, (m1, m2, w1, w2, x1, x2), {}, traffic, 60)


def late_kernel(scales, place, w1_ref, w2_ref, x1_ref, x2_ref, into1_ref, into2_ref, new_w1_ref, new_w2_ref):
    weight_block(w1_ref, x1_ref[...][None], new_w1_ref, scales[0])
    weight_block(w2_ref, x2_ref[...][None], new_w2_ref, scales[1])


def late_step(w1, w2, late, into1, into2, scales, owner, owners):
    rounds = w1.shape[0] // owners
    column = LATE[0] * w1.shape[2] // w2.shape[2]

    def specs(array, count, first_column):
        turn = lambda i: jnp.minimum(i, count - 1)
        return (pl.BlockSpec((1,) + array.shape[1:], lambda i, place: ((rounds - count + turn(i)) * owners + place[0], 0, 0)),
                pl.BlockSpec(array.shape[1:], lambda i, place: (0, first_column + turn(i))))

    (w1_spec, x1_spec), (w2_spec, x2_spec) = specs(w1, LATE[0], 0), specs(w2, LATE[1], column)
    return call_plain(functools.partial(late_kernel, scales), 'late', max(LATE),
                      [w1_spec, w2_spec, x1_spec, x2_spec] + [pl.BlockSpec(memory_space=pl.ANY)] * 2, [w1_spec, w2_spec],
                      [jax.ShapeDtypeStruct(w.shape, w.dtype) for w in (w1, w2)],
                      owner, (w1, w2, late, late, into1, into2), {5: 0, 6: 1}, 5 * late.size, 54)


def solution(mesh):
    data_size = mesh.shape['data']
    model_size = mesh.shape['model']
    owners = data_size * model_size
    block_spec = P('stage', 'data', 'model')

    def local_step(w_fc1, m_fc1, g_fc1, w_fc2, m_fc2, g_fc2):
        scales = [0.2 * math.sqrt(max(w.shape[1] * data_size, w.shape[2] * model_size)) for w in (w_fc1, w_fc2)]
        model, data = lax.axis_index('model'), lax.axis_index('data')
        pair = 3 - model * 2 - (data >> 1)
        new_m1, new_m2, back1, back2, late_a, late_b = exchange(m_fc1, g_fc1, m_fc2, g_fc2, owners)
        late_a = lax.ppermute(late_a, ('model', 'data'), [(i, i ^ 6) for i in range(owners)])
        late_b = lax.ppermute(late_b, ('model', 'data'), [(i, i ^ 7) for i in range(owners)])
        new_m1, new_m2, new_w1, new_w2 = early_step(new_m1, new_m2, w_fc1, w_fc2, back1, back2, scales, pair[None], owners)
        same = pair * 2 + (data & 1)
        cross = same ^ 1
        new_w1, new_w2 = late_step(w_fc1, w_fc2, late_a, new_w1, new_w2, scales, same[None], owners)
        new_w1, new_w2 = late_step(w_fc1, w_fc2, late_b, new_w1, new_w2, scales, cross[None], owners)
        return new_w1, new_m1, new_w2, new_m2

    return jax.shard_map(local_step, mesh=mesh, in_specs=(block_spec,) * 6, out_specs=(block_spec,) * 4, check_vma=False)
```

```python
import functools
import math
import jax
import jax.numpy as jnp
from jax import lax
from jax.experimental import pallas as pl
from jax.experimental.pallas import tpu as pltpu
from jax.sharding import PartitionSpec as P

NS_STEPS = 5
NS_COEF_A = 3.4445
NS_COEF_B = -4.7750
NS_COEF_C = 2.0315
MOMENTUM = 0.95
LEARN_RATE = 0.04
DECAY = 0.2
NORM_EPS = 1e-7

MESH_ID = pl.DeviceIdType.MESH
GRAM_BLOCK = 256
ROW_BLOCK = 512


def iterate(x_ref, gram_ref, poly_ref):
    rows, cols = x_ref.shape
    gram_block = min(GRAM_BLOCK, cols)
    row_block = min(ROW_BLOCK, rows)

    @pl.loop(0, NS_STEPS)
    def ns_step(_):
        @pl.loop(0, cols // gram_block)
        def gram(i):
            span = pl.ds(pl.multiple_of(i * gram_block, gram_block), gram_block)
            part = lax.dot_general(x_ref[:, span], x_ref[...], (((0,), (0,)), ((), ())), preferred_element_type=jnp.float32)
            gram_ref[span, :] = part.astype(jnp.bfloat16)

        @pl.loop(0, cols // gram_block)
        def poly(i):
            span = pl.ds(pl.multiple_of(i * gram_block, gram_block), gram_block)
            gram_rows = gram_ref[span, :]
            gram_sq = jnp.dot(gram_rows, gram_ref[...], preferred_element_type=jnp.float32)
            poly_ref[span, :] = (NS_COEF_B * gram_rows.astype(jnp.float32) + NS_COEF_C * gram_sq).astype(jnp.bfloat16)

        @pl.loop(0, rows // row_block)
        def update(i):
            span = pl.ds(pl.multiple_of(i * row_block, row_block), row_block)
            x_rows = x_ref[span, :]
            term = jnp.dot(x_rows, poly_ref[...], preferred_element_type=jnp.float32)
            x_ref[span, :] = (NS_COEF_A * x_rows.astype(jnp.float32) + term).astype(jnp.bfloat16)


def momentum_block(m_ref, g_ref, slot, low_ref, index, sq_ref, owner, k):
    new_mom = MOMENTUM * m_ref[slot] + g_ref[slot].astype(jnp.float32)
    m_ref[slot] = new_mom
    low_ref[index] = new_mom.astype(jnp.bfloat16)
    squares = new_mom * new_mom
    rows, cols = squares.shape
    part = jnp.sum(squares.reshape(rows // 8, 8, cols), axis=0)
    total = part[:, :128]
    for start in range(128, cols, 128):
        total = total + part[:, start:start + 128]
    sq_ref[owner, k] = total


AHEAD = 3
LATE = (2, 3)
DIAGONAL = 2


def exchange_kernel(m1, g1, m2, g2, new_m1, new_m2, back1, back2, late_a, late_b, late_c, low1, low2, x1, x2, sq1, sq2, sums1, sums2,
                    gram1, poly1, gram2, poly2, m_buf1, g_buf1, m_buf2, g_buf2,
                    fwd1, fwd2, got1, got2, ret1, ret2, done_sems, sq_send1, sq_send2, sq_got1, sq_got2,
                    m_sem1, g_sem1, m_sem2, g_sem2, out_sem1, out_sem2, late_sem):
    model = lax.axis_index('model')
    data = lax.axis_index('data')
    chip, core = data // 2, data % 2
    me = model * 4 + data
    owners = 8
    experts = m1.shape[0]
    rounds = experts // owners
    slots = m_buf1.shape[0]
    early1, early2 = (rounds - late for late in LATE)

    def peer(turn):
        code = owners - 1 - turn
        return (model + code // 4) % 2, ((chip + code // 2 % 2) % 2) * 2 + (core + code % 2) % 2

    def at(place):
        return dict(device_id=(0, place[0], place[1]), device_id_type=MESH_ID)

    def expert(step):
        peer_model, peer_data = peer(step % owners)
        return step // owners * owners + peer_model * 4 + peer_data

    stack1 = (m1, g1, m_buf1, g_buf1, m_sem1, g_sem1)
    stack2 = (m2, g2, m_buf2, g_buf2, m_sem2, g_sem2)

    def loads(stack, step):
        m, g, m_buf, g_buf, m_sem, g_sem = stack
        slot, index = step % slots, expert(step)
        return (pltpu.make_async_copy(m.at[index], m_buf.at[slot], m_sem.at[slot]),
                pltpu.make_async_copy(g.at[index], g_buf.at[slot], g_sem.at[slot]))

    def store(stack, new_m, out_sem, step):
        slot = step % slots
        return pltpu.make_async_copy(stack[2].at[slot], new_m.at[expert(step)], out_sem.at[slot])

    for stack in (stack2, stack1):
        for step in range(AHEAD):
            for load in loads(stack, step):
                load.start()

    barrier = pltpu.get_barrier_semaphore()
    for turn in range(owners - 1):
        pl.semaphore_signal(barrier, inc=1, **at(peer(turn)))
    pl.semaphore_wait(barrier, owners - 1)

    def window(x_ref, k, at_model, at_data):
        rows, cols = x_ref.shape[1] // 4, x_ref.shape[2] // 2
        return x_ref.at[k, pl.ds(pl.multiple_of(at_data * rows, rows), rows), pl.ds(pl.multiple_of(at_model * cols, cols), cols)]

    def forward_round(k, stack, new_m, out_sem, low_ref, x_ref, fwd, got, sq_ref, sums_ref, sq_send, sq_got):
        def send(turn):
            place = peer(turn)
            owner = place[0] * 4 + place[1]
            pltpu.make_async_remote_copy(sq_ref.at[owner, k], sums_ref.at[k, me], sq_send.at[k], sq_got.at[k], **at(place)).start()
            pltpu.make_async_remote_copy(low_ref.at[k * owners + owner], window(x_ref, k, model, data), fwd.at[k], got.at[k],
                                         **at(place)).start()

        @pl.loop(0, owners)
        def block(turn):
            step = k * owners + turn
            index = expert(step)
            for load in loads(stack, step):
                load.wait()
            momentum_block(stack[2], stack[3], step % slots, low_ref, index, sq_ref, index - k * owners, k)
            store(stack, new_m, out_sem, step).start()

            @pl.when(turn > 0)
            def send_before():
                send(turn - 1)

            @pl.when(step >= slots - AHEAD)
            def stored():
                store(stack, new_m, out_sem, step + AHEAD - slots).wait()

            @pl.when(step + AHEAD < experts)
            def prefetch():
                for load in loads(stack, step + AHEAD):
                    load.start()

        pltpu.make_async_copy(sq_ref.at[me, k], sums_ref.at[k, me], sq_got.at[k]).start()
        pltpu.make_async_copy(low_ref.at[k * owners + me], window(x_ref, k, model, data), got.at[k]).start()

    def return_round(k, x_ref, dst, sems, t, early, first_column):
        def give(turn):
            place = peer(turn)
            pltpu.make_async_remote_copy(window(x_ref, k, *place), dst.at[k * owners + me], sems.at[k], done_sems.at[t],
                                         **at(place)).start()

        @pl.when(k < early)
        def to_diagonal():
            for turn in range(DIAGONAL):
                give(turn)

        for turn in range(DIAGONAL, owners - 1):
            give(turn)
        pltpu.make_async_copy(window(x_ref, k, model, data), dst.at[k * owners + me], done_sems.at[t]).start()

        @pl.when(k >= early)
        def keep():
            cols = dst.shape[2]
            span = pl.ds(pl.multiple_of(first_column + (k - early) * cols, cols), cols)
            pltpu.make_async_copy(window(x_ref, k, *peer(1)), late_a.at[:, span], late_sem.at[0]).start()
            cross = window(x_ref, k, *peer(0))
            last = k == rounds - 1 if t == 0 else False

            @pl.when(jnp.logical_not(last))
            def keep_b():
                pltpu.make_async_copy(cross, late_b.at[:, span], late_sem.at[1]).start()

            if t == 0:
                @pl.when(last)
                def keep_c():
                    pltpu.make_async_copy(cross, late_c, late_sem.at[2]).start()

    def wait_bytes(ref, sem):
        pltpu.make_async_copy(ref, ref, sem).wait()

    def orthogonalize(k, x_ref, got, sums_ref, sq_got, gram_ref, poly_ref):
        wait_bytes(sums_ref.at[k], sq_got.at[k])
        wait_bytes(x_ref.at[k], got.at[k])
        norm = jnp.sqrt(jnp.sum(sums_ref[k])) + NORM_EPS
        rows = x_ref.shape[1]

        @pl.loop(0, rows // 256)
        def normalize(i):
            span = pl.ds(pl.multiple_of(i * 256, 256), 256)
            x_ref[k, span, :] = (x_ref[k, span, :].astype(jnp.float32) / norm).astype(jnp.bfloat16)

        iterate(x_ref.at[k], gram_ref, poly_ref)

    @pl.loop(0, rounds)
    def forward(k):
        forward_round(k, stack2, new_m2, out_sem2, low2, x2, fwd2, got2, sq2, sums2, sq_send2, sq_got2)
        forward_round(k, stack1, new_m1, out_sem1, low1, x1, fwd1, got1, sq1, sums1, sq_send1, sq_got1)

    cols1, cols2 = low1.shape[2], low2.shape[2]

    @pl.loop(0, rounds)
    def work(k):
        orthogonalize(k, x2, got2, sums2, sq_got2, gram2, poly2)
        return_round(k, x2, back2, ret2, 0, early2, LATE[0] * cols1)
        orthogonalize(k, x1, got1, sums1, sq_got1, gram1, poly1)
        return_round(k, x1, back1, ret1, 1, early1, 0)

    count = owners - 1
    for stack, new_m, out_sem in ((stack2, new_m2, out_sem2), (stack1, new_m1, out_sem1)):
        for step in range(experts + AHEAD - slots, experts):
            store(stack, new_m, out_sem, step).wait()

    @pl.loop(0, rounds)
    def finish(k):
        for low, sq, fwd, ret, sq_send, early in ((low2, sq2, fwd2, ret2, sq_send2, early2), (low1, sq1, fwd1, ret1, sq_send1, early1)):
            wait_bytes(sq.at[pl.ds(0, count), 0], sq_send.at[k])
            wait_bytes(low.at[pl.ds(0, count)], fwd.at[k])

            wait_bytes(low.at[pl.ds(0, count - DIAGONAL)], ret.at[k])

            @pl.when(k < early)
            def returned():
                wait_bytes(low.at[pl.ds(0, DIAGONAL)], ret.at[k])

    wait_bytes(back2.at[pl.ds(0, experts - LATE[1] * DIAGONAL)], done_sems.at[0])
    wait_bytes(back1.at[pl.ds(0, experts - LATE[0] * DIAGONAL)], done_sems.at[1])
    wait_bytes(late_a, late_sem.at[0])
    wait_bytes(late_b, late_sem.at[1])
    wait_bytes(late_c, late_sem.at[2])


def exchange(m1, g1, m2, g2, owners):
    experts, rows, cols1 = m1.shape
    cols2 = m2.shape[2]
    rounds = experts // owners
    slots = 2 * AHEAD
    any_spec = pl.BlockSpec(memory_space=pl.ANY)
    flops = 2 * rounds * NS_STEPS * sum(2 * 4 * rows * c * c + c ** 3 for c in (2 * cols1, 2 * cols2))
    low = jnp.bfloat16
    dma = pltpu.SemaphoreType.DMA
    results = [((experts, rows, cols1), jnp.float32), ((experts, rows, cols2), jnp.float32),
               ((experts, rows, cols1), low), ((experts, rows, cols2), low),
               ((rows, LATE[0] * cols1 + LATE[1] * cols2), low), ((rows, LATE[0] * cols1 + (LATE[1] - 1) * cols2), low),
               ((rows, cols2), low)]
    return pl.pallas_call(
        exchange_kernel,
        in_specs=[any_spec] * 4,
        out_specs=[any_spec] * len(results),
        out_shape=[jax.ShapeDtypeStruct(*result) for result in results],
        scratch_shapes=[
            pltpu.VMEM((experts, rows, cols1), low),
            pltpu.VMEM((experts, rows, cols2), low),
            pltpu.VMEM((rounds, 4 * rows, 2 * cols1), low),
            pltpu.VMEM((rounds, 4 * rows, 2 * cols2), low),
            pltpu.VMEM((owners, rounds, 8, 128), jnp.float32),
            pltpu.VMEM((owners, rounds, 8, 128), jnp.float32),
            pltpu.VMEM((rounds, owners, 8, 128), jnp.float32),
            pltpu.VMEM((rounds, owners, 8, 128), jnp.float32),
            pltpu.VMEM((2 * cols1, 2 * cols1), low),
            pltpu.VMEM((2 * cols1, 2 * cols1), low),
            pltpu.VMEM((2 * cols2, 2 * cols2), low),
            pltpu.VMEM((2 * cols2, 2 * cols2), low),
            pltpu.VMEM((slots, rows, cols1), jnp.float32),
            pltpu.VMEM((slots, rows, cols1), low),
            pltpu.VMEM((slots, rows, cols2), jnp.float32),
            pltpu.VMEM((slots, rows, cols2), low),
        ] + [dma((rounds,))] * 6 + [dma((2,))] + [dma((rounds,))] * 4 + [dma((slots,))] * 6 + [dma((3,))],
        compiler_params=pltpu.CompilerParams(collective_id=0, has_side_effects=True, vmem_limit_bytes=62 * 2 ** 20),
        cost_estimate=pl.CostEstimate(flops=flops, bytes_accessed=14 * (m1.size + m2.size), transcendentals=0),
        name='exchange',
    )(m1, g1, m2, g2)


def call_plain(kernel, name, steps, in_specs, out_specs, out_shape, place, args, aliases, traffic, limit):
    return pl.pallas_call(
        kernel,
        grid_spec=pltpu.PrefetchScalarGridSpec(num_scalar_prefetch=1, grid=(steps,), in_specs=in_specs, out_specs=out_specs),
        out_shape=out_shape, input_output_aliases=aliases,
        compiler_params=pltpu.CompilerParams(dimension_semantics=('arbitrary',), vmem_limit_bytes=limit * 2 ** 20),
        cost_estimate=pl.CostEstimate(flops=traffic, bytes_accessed=traffic, transcendentals=0),
        name=name,
    )(place, *args)


def weight_block(w_ref, x_mat, out_ref, scale):
    w_old = w_ref[...]
    out_ref[...] = w_old - LEARN_RATE * (x_mat.astype(jnp.float32) * scale + DECAY * w_old)


def early_kernel(scales, place, m1_ref, m2_ref, w1_ref, w2_ref, x1_ref, x2_ref, new_m1_ref, new_m2_ref, new_w1_ref, new_w2_ref):
    new_m1_ref[...] = m1_ref[...]
    new_m2_ref[...] = m2_ref[...]
    weight_block(w1_ref, x1_ref[...], new_w1_ref, scales[0])
    weight_block(w2_ref, x2_ref[...], new_w2_ref, scales[1])


def early_step(m1, m2, w1, w2, x1, x2, scales, pair, owners):
    steps, pairs = m1.shape[0] // 2, owners // 2

    def spec(array, late):
        def turn(i, place):
            other = (place[0] + 1 + jnp.minimum(i % pairs, pairs - 2)) % pairs
            return jnp.where(i < steps - late * pairs, i, i // pairs * pairs + other), 0, 0

        return pl.BlockSpec((2,) + array.shape[1:], turn)

    m_specs = [pl.BlockSpec((2,) + m.shape[1:], lambda i, place: (i, 0, 0)) for m in (m1, m2)]
    w_specs = [spec(w, late) for w, late in zip((w1, w2), LATE)]
    outs = [jax.ShapeDtypeStruct(array.shape, array.dtype) for array in (m1, m2, w1, w2)]
    traffic = 18 * (m1.size + m2.size)
    return call_plain(functools.partial(early_kernel, scales), 'early', steps, m_specs + w_specs + w_specs, m_specs + w_specs,
                      outs, pair, (m1, m2, w1, w2, x1, x2), {}, traffic, 60)


def late_kernel(scales, jobs, place, w1_ref, w2_ref, *refs):
    sources, refs = refs[:len(jobs)], refs[len(jobs) + 2:]
    outs, bufs, load_sems, store_sems = refs[:2], refs[2:4], refs[4], refs[5]
    work, loads, used = [], [], [0, 0]
    for (which, blocks), source in zip(jobs, sources):
        for stack, first_expert, column in blocks:
            slot = used[stack]
            used[stack] += 1
            index = first_expert + (place[0] ^ which)
            buf = bufs[stack].at[slot]
            load = pltpu.make_async_copy((w1_ref, w2_ref)[stack].at[index], buf, load_sems.at[stack, slot])
            load.start()
            work.append((load, pltpu.make_async_copy(buf, outs[stack].at[index], store_sems.at[stack, slot]),
                         buf, source.at[:, pl.ds(column, buf.shape[1])], scales[stack]))
    for load, store, buf, x_ref, scale in work:
        load.wait()
        weight_block(buf, x_ref[...], buf, scale)
        store.start()
    for _, store, _, _, _ in work:
        store.wait()


def late_step(w1, w2, into1, into2, scales, place, jobs):
    any_spec, vmem_spec = pl.BlockSpec(memory_space=pl.ANY), pl.BlockSpec(memory_space=pltpu.VMEM)
    count = [max(1, sum(block[0] == stack for job in jobs for block in job[2])) for stack in range(2)]
    held = [pltpu.with_memory_space_constraint(w, pltpu.HBM) for w in (w1, w2)]
    arrays = [job[0] for job in jobs]
    traffic = 5 * sum(array.size for array in arrays)
    return pl.pallas_call(
        functools.partial(late_kernel, scales, [job[1:] for job in jobs]),
        in_specs=[pl.BlockSpec(memory_space=pltpu.SMEM)] + [any_spec] * 2 + [vmem_spec] * len(jobs) + [any_spec] * 2,
        out_specs=[any_spec] * 2,
        out_shape=[jax.ShapeDtypeStruct(w.shape, w.dtype) for w in (w1, w2)],
        scratch_shapes=[pltpu.VMEM((n,) + w.shape[1:], w.dtype) for n, w in zip(count, (w1, w2))]
        + [pltpu.SemaphoreType.DMA((2, max(count)))] * 2,
        input_output_aliases={3 + len(jobs): 0, 4 + len(jobs): 1},
        compiler_params=pltpu.CompilerParams(vmem_limit_bytes=24 * 2 ** 20),
        cost_estimate=pl.CostEstimate(flops=traffic, bytes_accessed=2 * traffic, transcendentals=0),
        name='late',
    )(place, *held, *arrays, into1, into2)


def solution(mesh):
    data_size = mesh.shape['data']
    model_size = mesh.shape['model']
    owners = data_size * model_size
    block_spec = P('stage', 'data', 'model')

    def local_step(w_fc1, m_fc1, g_fc1, w_fc2, m_fc2, g_fc2):
        scales = [0.2 * math.sqrt(max(w.shape[1] * data_size, w.shape[2] * model_size)) for w in (w_fc1, w_fc2)]
        model, data = lax.axis_index('model'), lax.axis_index('data')
        pair = 3 - model * 2 - (data >> 1)
        same = pair * 2 + (data & 1)
        new_m1, new_m2, back1, back2, late_a, late_b, late_c = exchange(m_fc1, g_fc1, m_fc2, g_fc2, owners)
        late_a = lax.ppermute(late_a, ('model', 'data'), [(i, i ^ 6) for i in range(owners)])
        late_b = lax.ppermute(late_b, ('model', 'data'), [(i, i ^ 7) for i in range(owners)])
        late_c = lax.ppermute(late_c, ('model', 'data'), [(i, i ^ 7) for i in range(owners)])
        new_m1, new_m2, new_w1, new_w2 = early_step(new_m1, new_m2, w_fc1, w_fc2, back1, back2, scales, pair[None], owners)
        experts, (cols1, cols2) = w_fc1.shape[0], (w_fc1.shape[2], w_fc2.shape[2])
        blocks = [(0, experts - (LATE[0] - i) * owners, i * cols1) for i in range(LATE[0])]
        blocks += [(1, experts - (LATE[1] - i) * owners, LATE[0] * cols1 + i * cols2) for i in range(LATE[1])]
        new_w1, new_w2 = late_step(w_fc1, w_fc2, new_w1, new_w2, scales, same[None], [(late_a, 0, blocks), (late_b, 1, blocks[:-1])])
        new_w1, new_w2 = late_step(w_fc1, w_fc2, new_w1, new_w2, scales, same[None], [(late_c, 1, [(1, experts - owners, 0)])])
        return new_w1, new_m1, new_w2, new_m2

    return jax.shard_map(local_step, mesh=mesh, in_specs=(block_spec,) * 6, out_specs=(block_spec,) * 4, check_vma=False)
```

```python
import functools
import math
import jax
import jax.numpy as jnp
from jax import lax
from jax.experimental import pallas as pl
from jax.experimental.pallas import tpu as pltpu
from jax.sharding import PartitionSpec as P

NS_STEPS = 5
NS_COEF_A = 3.4445
NS_COEF_B = -4.7750
NS_COEF_C = 2.0315
MOMENTUM = 0.95
LEARN_RATE = 0.04
DECAY = 0.2
NORM_EPS = 1e-7

MESH_ID = pl.DeviceIdType.MESH
GRAM_BLOCK = 256
ROW_BLOCK = 512


def iterate(x_ref, gram_ref, poly_ref):
    rows, cols = x_ref.shape
    gram_block = min(GRAM_BLOCK, cols)
    row_block = min(ROW_BLOCK, rows)

    @pl.loop(0, NS_STEPS)
    def ns_step(_):
        @pl.loop(0, cols // gram_block)
        def gram(i):
            span = pl.ds(pl.multiple_of(i * gram_block, gram_block), gram_block)
            part = lax.dot_general(x_ref[:, span], x_ref[...], (((0,), (0,)), ((), ())), preferred_element_type=jnp.float32)
            gram_ref[span, :] = part.astype(jnp.bfloat16)

        @pl.loop(0, cols // gram_block)
        def poly(i):
            span = pl.ds(pl.multiple_of(i * gram_block, gram_block), gram_block)
            gram_rows = gram_ref[span, :]
            gram_sq = jnp.dot(gram_rows, gram_ref[...], preferred_element_type=jnp.float32)
            poly_ref[span, :] = (NS_COEF_B * gram_rows.astype(jnp.float32) + NS_COEF_C * gram_sq).astype(jnp.bfloat16)

        @pl.loop(0, rows // row_block)
        def update(i):
            span = pl.ds(pl.multiple_of(i * row_block, row_block), row_block)
            x_rows = x_ref[span, :]
            term = jnp.dot(x_rows, poly_ref[...], preferred_element_type=jnp.float32)
            x_ref[span, :] = (NS_COEF_A * x_rows.astype(jnp.float32) + term).astype(jnp.bfloat16)


def momentum_block(m_ref, g_ref, slot, low_ref, index, sq_ref, owner, k):
    new_mom = MOMENTUM * m_ref[slot] + g_ref[slot].astype(jnp.float32)
    m_ref[slot] = new_mom
    low_ref[index] = new_mom.astype(jnp.bfloat16)
    squares = new_mom * new_mom
    rows, cols = squares.shape
    part = jnp.sum(squares.reshape(rows // 8, 8, cols), axis=0)
    total = part[:, :128]
    for start in range(128, cols, 128):
        total = total + part[:, start:start + 128]
    sq_ref[owner, k] = total


AHEAD = 3
FIRST = 2
LATE = (2, 3)
DIAGONAL = 2


def exchange_kernel(m1, g1, m2, g2, new_m1, new_m2, back1, back2, late_a, late_b, late_c, low1, low2, x1, x2, sq1, sq2, sums1, sums2,
                    gram1, poly1, gram2, poly2, m_buf1, g_buf1, m_buf2, g_buf2,
                    fwd1, fwd2, got1, got2, ret1, ret2, done_sems, sq_send1, sq_send2, sq_got1, sq_got2,
                    m_sem1, g_sem1, m_sem2, g_sem2, out_sem1, out_sem2, late_sem):
    model = lax.axis_index('model')
    data = lax.axis_index('data')
    chip, core = data // 2, data % 2
    me = model * 4 + data
    owners = 8
    experts = m1.shape[0]
    rounds = experts // owners
    slots = m_buf1.shape[0]
    early1, early2 = (rounds - late for late in LATE)

    def peer(turn):
        code = owners - 1 - turn
        return (model + code // 4) % 2, ((chip + code // 2 % 2) % 2) * 2 + (core + code % 2) % 2

    def at(place):
        return dict(device_id=(0, place[0], place[1]), device_id_type=MESH_ID)

    def expert(step):
        peer_model, peer_data = peer(step % owners)
        return step // owners * owners + peer_model * 4 + peer_data

    stack1 = (m1, g1, m_buf1, g_buf1, m_sem1, g_sem1)
    stack2 = (m2, g2, m_buf2, g_buf2, m_sem2, g_sem2)

    def loads(stack, step):
        m, g, m_buf, g_buf, m_sem, g_sem = stack
        slot, index = step % slots, expert(step)
        return (pltpu.make_async_copy(m.at[index], m_buf.at[slot], m_sem.at[slot]),
                pltpu.make_async_copy(g.at[index], g_buf.at[slot], g_sem.at[slot]))

    def store(stack, new_m, out_sem, step):
        slot = step % slots
        return pltpu.make_async_copy(stack[2].at[slot], new_m.at[expert(step)], out_sem.at[slot])

    for stack in (stack2, stack1):
        for step in range(AHEAD):
            for load in loads(stack, step):
                load.start()

    barrier = pltpu.get_barrier_semaphore()
    for turn in range(owners - 1):
        pl.semaphore_signal(barrier, inc=1, **at(peer(turn)))

    def compute(step, stack, new_m, out_sem, low_ref, sq_ref):
        for load in loads(stack, step):
            load.wait()
        index = expert(step)
        momentum_block(stack[2], stack[3], step % slots, low_ref, index, sq_ref, index % owners, step // owners)
        store(stack, new_m, out_sem, step).start()

    for step in range(FIRST):
        compute(step, stack2, new_m2, out_sem2, low2, sq2)

    pl.semaphore_wait(barrier, owners - 1)

    def window(x_ref, k, at_model, at_data):
        rows, cols = x_ref.shape[1] // 4, x_ref.shape[2] // 2
        return x_ref.at[k, pl.ds(pl.multiple_of(at_data * rows, rows), rows), pl.ds(pl.multiple_of(at_model * cols, cols), cols)]

    def forward_round(k, computed, stack, new_m, out_sem, low_ref, x_ref, fwd, got, sq_ref, sums_ref, sq_send, sq_got):
        def send(turn):
            place = peer(turn)
            owner = place[0] * 4 + place[1]
            pltpu.make_async_remote_copy(sq_ref.at[owner, k], sums_ref.at[k, me], sq_send.at[k], sq_got.at[k], **at(place)).start()
            pltpu.make_async_remote_copy(low_ref.at[k * owners + owner], window(x_ref, k, model, data), fwd.at[k], got.at[k],
                                         **at(place)).start()

        @pl.loop(0, owners)
        def block(turn):
            step = k * owners + turn

            @pl.when(step >= computed)
            def compute_now():
                compute(step, stack, new_m, out_sem, low_ref, sq_ref)

            @pl.when(turn > 0)
            def send_before():
                send(turn - 1)

            @pl.when(step >= slots - AHEAD)
            def stored():
                store(stack, new_m, out_sem, step + AHEAD - slots).wait()

            @pl.when(step + AHEAD < experts)
            def prefetch():
                for load in loads(stack, step + AHEAD):
                    load.start()

        pltpu.make_async_copy(sq_ref.at[me, k], sums_ref.at[k, me], sq_got.at[k]).start()
        pltpu.make_async_copy(low_ref.at[k * owners + me], window(x_ref, k, model, data), got.at[k]).start()

    def return_round(k, x_ref, dst, sems, t, early, first_column):
        def give(turn):
            place = peer(turn)
            pltpu.make_async_remote_copy(window(x_ref, k, *place), dst.at[k * owners + me], sems.at[k], done_sems.at[t],
                                         **at(place)).start()

        @pl.when(k < early)
        def to_diagonal():
            for turn in range(DIAGONAL):
                give(turn)

        for turn in range(DIAGONAL, owners - 1):
            give(turn)
        pltpu.make_async_copy(window(x_ref, k, model, data), dst.at[k * owners + me], done_sems.at[t]).start()

        @pl.when(k >= early)
        def keep():
            cols = dst.shape[2]
            span = pl.ds(pl.multiple_of(first_column + (k - early) * cols, cols), cols)
            pltpu.make_async_copy(window(x_ref, k, *peer(1)), late_a.at[:, span], late_sem.at[0]).start()
            cross = window(x_ref, k, *peer(0))
            last = k == rounds - 1 if t == 0 else False

            @pl.when(jnp.logical_not(last))
            def keep_b():
                pltpu.make_async_copy(cross, late_b.at[:, span], late_sem.at[1]).start()

            if t == 0:
                @pl.when(last)
                def keep_c():
                    pltpu.make_async_copy(cross, late_c, late_sem.at[2]).start()

    def wait_bytes(ref, sem):
        pltpu.make_async_copy(ref, ref, sem).wait()

    def orthogonalize(k, x_ref, got, sums_ref, sq_got, gram_ref, poly_ref):
        wait_bytes(sums_ref.at[k], sq_got.at[k])
        wait_bytes(x_ref.at[k], got.at[k])
        norm = jnp.sqrt(jnp.sum(sums_ref[k])) + NORM_EPS
        rows = x_ref.shape[1]

        @pl.loop(0, rows // 256)
        def normalize(i):
            span = pl.ds(pl.multiple_of(i * 256, 256), 256)
            x_ref[k, span, :] = (x_ref[k, span, :].astype(jnp.float32) / norm).astype(jnp.bfloat16)

        iterate(x_ref.at[k], gram_ref, poly_ref)

    @pl.loop(0, rounds)
    def forward(k):
        forward_round(k, FIRST, stack2, new_m2, out_sem2, low2, x2, fwd2, got2, sq2, sums2, sq_send2, sq_got2)
        forward_round(k, 0, stack1, new_m1, out_sem1, low1, x1, fwd1, got1, sq1, sums1, sq_send1, sq_got1)

    cols1, cols2 = low1.shape[2], low2.shape[2]

    @pl.loop(0, rounds)
    def work(k):
        orthogonalize(k, x2, got2, sums2, sq_got2, gram2, poly2)
        return_round(k, x2, back2, ret2, 0, early2, LATE[0] * cols1)
        orthogonalize(k, x1, got1, sums1, sq_got1, gram1, poly1)
        return_round(k, x1, back1, ret1, 1, early1, 0)

    count = owners - 1
    for stack, new_m, out_sem in ((stack2, new_m2, out_sem2), (stack1, new_m1, out_sem1)):
        for step in range(experts + AHEAD - slots, experts):
            store(stack, new_m, out_sem, step).wait()

    @pl.loop(0, rounds)
    def finish(k):
        for low, sq, fwd, ret, sq_send, early in ((low2, sq2, fwd2, ret2, sq_send2, early2), (low1, sq1, fwd1, ret1, sq_send1, early1)):
            wait_bytes(sq.at[pl.ds(0, count), 0], sq_send.at[k])
            wait_bytes(low.at[pl.ds(0, count)], fwd.at[k])

            wait_bytes(low.at[pl.ds(0, count - DIAGONAL)], ret.at[k])

            @pl.when(k < early)
            def returned():
                wait_bytes(low.at[pl.ds(0, DIAGONAL)], ret.at[k])

    wait_bytes(back2.at[pl.ds(0, experts - LATE[1] * DIAGONAL)], done_sems.at[0])
    wait_bytes(back1.at[pl.ds(0, experts - LATE[0] * DIAGONAL)], done_sems.at[1])
    wait_bytes(late_a, late_sem.at[0])
    wait_bytes(late_b, late_sem.at[1])
    wait_bytes(late_c, late_sem.at[2])


def exchange(m1, g1, m2, g2, owners):
    experts, rows, cols1 = m1.shape
    cols2 = m2.shape[2]
    rounds = experts // owners
    slots = 2 * AHEAD
    any_spec = pl.BlockSpec(memory_space=pl.ANY)
    flops = 2 * rounds * NS_STEPS * sum(2 * 4 * rows * c * c + c ** 3 for c in (2 * cols1, 2 * cols2))
    low = jnp.bfloat16
    dma = pltpu.SemaphoreType.DMA
    results = [((experts, rows, cols1), jnp.float32), ((experts, rows, cols2), jnp.float32),
               ((experts, rows, cols1), low), ((experts, rows, cols2), low),
               ((rows, LATE[0] * cols1 + LATE[1] * cols2), low), ((rows, LATE[0] * cols1 + (LATE[1] - 1) * cols2), low),
               ((rows, cols2), low)]
    return pl.pallas_call(
        exchange_kernel,
        in_specs=[any_spec] * 4,
        out_specs=[any_spec] * len(results),
        out_shape=[jax.ShapeDtypeStruct(*result) for result in results],
        scratch_shapes=[
            pltpu.VMEM((experts, rows, cols1), low),
            pltpu.VMEM((experts, rows, cols2), low),
            pltpu.VMEM((rounds, 4 * rows, 2 * cols1), low),
            pltpu.VMEM((rounds, 4 * rows, 2 * cols2), low),
            pltpu.VMEM((owners, rounds, 8, 128), jnp.float32),
            pltpu.VMEM((owners, rounds, 8, 128), jnp.float32),
            pltpu.VMEM((rounds, owners, 8, 128), jnp.float32),
            pltpu.VMEM((rounds, owners, 8, 128), jnp.float32),
            pltpu.VMEM((2 * cols1, 2 * cols1), low),
            pltpu.VMEM((2 * cols1, 2 * cols1), low),
            pltpu.VMEM((2 * cols2, 2 * cols2), low),
            pltpu.VMEM((2 * cols2, 2 * cols2), low),
            pltpu.VMEM((slots, rows, cols1), jnp.float32),
            pltpu.VMEM((slots, rows, cols1), low),
            pltpu.VMEM((slots, rows, cols2), jnp.float32),
            pltpu.VMEM((slots, rows, cols2), low),
        ] + [dma((rounds,))] * 6 + [dma((2,))] + [dma((rounds,))] * 4 + [dma((slots,))] * 6 + [dma((3,))],
        compiler_params=pltpu.CompilerParams(collective_id=0, has_side_effects=True, vmem_limit_bytes=62 * 2 ** 20),
        cost_estimate=pl.CostEstimate(flops=flops, bytes_accessed=14 * (m1.size + m2.size), transcendentals=0),
        name='exchange',
    )(m1, g1, m2, g2)


def call_plain(kernel, name, steps, in_specs, out_specs, out_shape, place, args, aliases, traffic, limit):
    return pl.pallas_call(
        kernel,
        grid_spec=pltpu.PrefetchScalarGridSpec(num_scalar_prefetch=1, grid=(steps,), in_specs=in_specs, out_specs=out_specs),
        out_shape=out_shape, input_output_aliases=aliases,
        compiler_params=pltpu.CompilerParams(dimension_semantics=('arbitrary',), vmem_limit_bytes=limit * 2 ** 20),
        cost_estimate=pl.CostEstimate(flops=traffic, bytes_accessed=traffic, transcendentals=0),
        name=name,
    )(place, *args)


def weight_block(w_ref, x_mat, out_ref, scale):
    w_old = w_ref[...]
    out_ref[...] = w_old - LEARN_RATE * (x_mat.astype(jnp.float32) * scale + DECAY * w_old)


def early_kernel(scales, place, m1_ref, m2_ref, w1_ref, w2_ref, x1_ref, x2_ref, new_m1_ref, new_m2_ref, new_w1_ref, new_w2_ref):
    new_m1_ref[...] = m1_ref[...]
    new_m2_ref[...] = m2_ref[...]
    weight_block(w1_ref, x1_ref[...], new_w1_ref, scales[0])
    weight_block(w2_ref, x2_ref[...], new_w2_ref, scales[1])


def early_step(m1, m2, w1, w2, x1, x2, scales, pair, owners):
    steps, pairs = m1.shape[0] // 2, owners // 2

    def spec(array, late):
        def turn(i, place):
            other = (place[0] + 1 + jnp.minimum(i % pairs, pairs - 2)) % pairs
            return jnp.where(i < steps - late * pairs, i, i // pairs * pairs + other), 0, 0

        return pl.BlockSpec((2,) + array.shape[1:], turn)

    m_specs = [pl.BlockSpec((2,) + m.shape[1:], lambda i, place: (i, 0, 0)) for m in (m1, m2)]
    w_specs = [spec(w, late) for w, late in zip((w1, w2), LATE)]
    outs = [jax.ShapeDtypeStruct(array.shape, array.dtype) for array in (m1, m2, w1, w2)]
    traffic = 18 * (m1.size + m2.size)
    return call_plain(functools.partial(early_kernel, scales), 'early', steps, m_specs + w_specs + w_specs, m_specs + w_specs,
                      outs, pair, (m1, m2, w1, w2, x1, x2), {}, traffic, 60)


def late_kernel(scales, jobs, given, keep, place, w1_ref, w2_ref, *refs):
    given_refs, refs = refs[:given], refs[given:]
    sources, refs = refs[:len(jobs)], refs[len(jobs) + 2:]
    outs, kept, refs = refs[:2], refs[2:2 + len(keep)], refs[2 + len(keep):]
    bufs, (load_sems, store_sems, keep_sem) = refs[:2], refs[2:]
    w_refs = w1_ref, w2_ref
    keeps = [pltpu.make_async_copy(w_refs[stack].at[first_expert + (place[0] ^ which)], ref.at[0], keep_sem)
             for (stack, first_expert, which), ref in zip(keep, kept)]
    work, used = [], [0, 0]
    for (which, blocks), source in zip(jobs, sources):
        for stack, first_expert, column in blocks:
            slot = used[stack]
            used[stack] += 1
            index = first_expert + (place[0] ^ which)
            buf = bufs[stack].at[slot]
            load = None if given else pltpu.make_async_copy(w_refs[stack].at[index], buf, load_sems.at[stack, slot])
            if load is not None:
                load.start()
            work.append((load, pltpu.make_async_copy(buf, outs[stack].at[index], store_sems.at[stack, slot]),
                         buf, source.at[:, pl.ds(column, buf.shape[1])], scales[stack]))
    for copy in keeps:
        copy.start()
    for load, store, buf, x_ref, scale in work:
        if load is not None:
            load.wait()
        weight_block(given_refs[0].at[0] if given else buf, x_ref[...], buf, scale)
        store.start()
    for _, store, _, _, _ in work:
        store.wait()
    for copy in keeps:
        copy.wait()


def late_step(w1, w2, into1, into2, scales, place, jobs, given=(), keep=()):
    any_spec, vmem_spec = pl.BlockSpec(memory_space=pl.ANY), pl.BlockSpec(memory_space=pltpu.VMEM)
    count = [max(1, sum(block[0] == stack for job in jobs for block in job[2])) for stack in range(2)]
    held = [pltpu.with_memory_space_constraint(w, pltpu.HBM) for w in (w1, w2)]
    arrays = [job[0] for job in jobs]
    traffic = 5 * sum(array.size for array in arrays)
    before = 3 + len(given) + len(jobs)
    return pl.pallas_call(
        functools.partial(late_kernel, scales, [job[1:] for job in jobs], len(given), keep),
        in_specs=[pl.BlockSpec(memory_space=pltpu.SMEM)] + [any_spec] * 2 + [vmem_spec] * (before - 3) + [any_spec] * 2,
        out_specs=[any_spec] * (2 + len(keep)),
        out_shape=[jax.ShapeDtypeStruct(w.shape, w.dtype) for w in (w1, w2)]
        + [jax.ShapeDtypeStruct((1,) + (w1, w2)[stack].shape[1:], w1.dtype) for stack, _, _ in keep],
        scratch_shapes=[pltpu.VMEM((n,) + w.shape[1:], w.dtype) for n, w in zip(count, (w1, w2))]
        + [pltpu.SemaphoreType.DMA((2, max(count)))] * 2 + [pltpu.SemaphoreType.DMA],
        input_output_aliases={before: 0, before + 1: 1},
        compiler_params=pltpu.CompilerParams(vmem_limit_bytes=24 * 2 ** 20),
        cost_estimate=pl.CostEstimate(flops=traffic, bytes_accessed=2 * traffic, transcendentals=0),
        name='late',
    )(place, *held, *given, *arrays, into1, into2)


def solution(mesh):
    data_size = mesh.shape['data']
    model_size = mesh.shape['model']
    owners = data_size * model_size
    block_spec = P('stage', 'data', 'model')

    def local_step(w_fc1, m_fc1, g_fc1, w_fc2, m_fc2, g_fc2):
        scales = [0.2 * math.sqrt(max(w.shape[1] * data_size, w.shape[2] * model_size)) for w in (w_fc1, w_fc2)]
        model, data = lax.axis_index('model'), lax.axis_index('data')
        pair = 3 - model * 2 - (data >> 1)
        same = pair * 2 + (data & 1)
        new_m1, new_m2, back1, back2, late_a, late_b, late_c = exchange(m_fc1, g_fc1, m_fc2, g_fc2, owners)
        late_a = lax.ppermute(late_a, ('model', 'data'), [(i, i ^ 6) for i in range(owners)])
        late_b = lax.ppermute(late_b, ('model', 'data'), [(i, i ^ 7) for i in range(owners)])
        late_c = lax.ppermute(late_c, ('model', 'data'), [(i, i ^ 7) for i in range(owners)])
        new_m1, new_m2, new_w1, new_w2 = early_step(new_m1, new_m2, w_fc1, w_fc2, back1, back2, scales, pair[None], owners)
        experts, (cols1, cols2) = w_fc1.shape[0], (w_fc1.shape[2], w_fc2.shape[2])
        blocks = [(0, experts - (LATE[0] - i) * owners, i * cols1) for i in range(LATE[0])]
        blocks += [(1, experts - (LATE[1] - i) * owners, LATE[0] * cols1 + i * cols2) for i in range(LATE[1])]
        new_w1, new_w2, w_last = late_step(w_fc1, w_fc2, new_w1, new_w2, scales, same[None],
                                           [(late_a, 0, blocks), (late_b, 1, blocks[:-1])], keep=[(1, experts - owners, 1)])
        new_w1, new_w2 = late_step(w_fc1, w_fc2, new_w1, new_w2, scales, same[None],
                                   [(late_c, 1, [(1, experts - owners, 0)])], given=[w_last])
        return new_w1, new_m1, new_w2, new_m2

    return jax.shard_map(local_step, mesh=mesh, in_specs=(block_spec,) * 6, out_specs=(block_spec,) * 4, check_vma=False)
```

```python
import functools
import math
import jax
import jax.numpy as jnp
from jax import lax
from jax.experimental import pallas as pl
from jax.experimental.pallas import tpu as pltpu
from jax.sharding import PartitionSpec as P

NS_STEPS = 5
NS_COEF_A = 3.4445
NS_COEF_B = -4.7750
NS_COEF_C = 2.0315
MOMENTUM = 0.95
LEARN_RATE = 0.04
DECAY = 0.2
NORM_EPS = 1e-7

MESH_ID = pl.DeviceIdType.MESH
GRAM_BLOCK = 256
ROW_BLOCK = 512


def iterate(x_ref, gram_ref, poly_ref):
    rows, cols = x_ref.shape
    gram_block = min(GRAM_BLOCK, cols)
    row_block = min(ROW_BLOCK, rows)

    @pl.loop(0, NS_STEPS)
    def ns_step(_):
        @pl.loop(0, cols // gram_block)
        def gram(i):
            span = pl.ds(pl.multiple_of(i * gram_block, gram_block), gram_block)
            part = lax.dot_general(x_ref[:, span], x_ref[...], (((0,), (0,)), ((), ())), preferred_element_type=jnp.float32)
            gram_ref[span, :] = part.astype(jnp.bfloat16)

        @pl.loop(0, cols // gram_block)
        def poly(i):
            span = pl.ds(pl.multiple_of(i * gram_block, gram_block), gram_block)
            gram_rows = gram_ref[span, :]
            gram_sq = jnp.dot(gram_rows, gram_ref[...], preferred_element_type=jnp.float32)
            poly_ref[span, :] = (NS_COEF_B * gram_rows.astype(jnp.float32) + NS_COEF_C * gram_sq).astype(jnp.bfloat16)

        @pl.loop(0, rows // row_block)
        def update(i):
            span = pl.ds(pl.multiple_of(i * row_block, row_block), row_block)
            x_rows = x_ref[span, :]
            term = jnp.dot(x_rows, poly_ref[...], preferred_element_type=jnp.float32)
            x_ref[span, :] = (NS_COEF_A * x_rows.astype(jnp.float32) + term).astype(jnp.bfloat16)


def momentum_block(m_ref, g_ref, slot, low_ref, index, sq_ref, owner, k):
    new_mom = MOMENTUM * m_ref[slot] + g_ref[slot].astype(jnp.float32)
    m_ref[slot] = new_mom
    low_ref[index] = new_mom.astype(jnp.bfloat16)
    squares = new_mom * new_mom
    rows, cols = squares.shape
    part = jnp.sum(squares.reshape(rows // 8, 8, cols), axis=0)
    total = part[:, :128]
    for start in range(128, cols, 128):
        total = total + part[:, start:start + 128]
    sq_ref[owner, k] = total


AHEAD = 3
FIRST = 2
LATE = (2, 3)
DIAGONAL = 2


def exchange_kernel(m1, g1, m2, g2, new_m1, new_m2, back1, back2, late_a, late_b, late_c, low1, low2, x1, x2, sq1, sq2, sums1, sums2,
                    gram1, poly1, gram2, poly2, m_buf1, g_buf1, m_buf2, g_buf2,
                    fwd1, fwd2, got1, got2, ret1, ret2, done_sems, sq_send1, sq_send2, sq_got1, sq_got2,
                    m_sem1, g_sem1, m_sem2, g_sem2, out_sem1, out_sem2, late_sem):
    model = lax.axis_index('model')
    data = lax.axis_index('data')
    chip, core = data // 2, data % 2
    me = model * 4 + data
    owners = 8
    experts = m1.shape[0]
    rounds = experts // owners
    slots = m_buf1.shape[0]
    early1, early2 = (rounds - late for late in LATE)

    def peer(turn):
        code = owners - 1 - turn
        return (model + code // 4) % 2, ((chip + code // 2 % 2) % 2) * 2 + (core + code % 2) % 2

    def at(place):
        return dict(device_id=(0, place[0], place[1]), device_id_type=MESH_ID)

    def expert(step):
        peer_model, peer_data = peer(step % owners)
        return step // owners * owners + peer_model * 4 + peer_data

    stack1 = (m1, g1, m_buf1, g_buf1, m_sem1, g_sem1)
    stack2 = (m2, g2, m_buf2, g_buf2, m_sem2, g_sem2)

    def loads(stack, step):
        m, g, m_buf, g_buf, m_sem, g_sem = stack
        slot, index = step % slots, expert(step)
        return (pltpu.make_async_copy(m.at[index], m_buf.at[slot], m_sem.at[slot]),
                pltpu.make_async_copy(g.at[index], g_buf.at[slot], g_sem.at[slot]))

    def store(stack, new_m, out_sem, step):
        slot = step % slots
        return pltpu.make_async_copy(stack[2].at[slot], new_m.at[expert(step)], out_sem.at[slot])

    for stack in (stack2, stack1):
        for step in range(AHEAD):
            for load in loads(stack, step):
                load.start()

    barrier = pltpu.get_barrier_semaphore()
    for turn in range(owners - 1):
        pl.semaphore_signal(barrier, inc=1, **at(peer(turn)))

    def compute(step, stack, new_m, out_sem, low_ref, sq_ref):
        for load in loads(stack, step):
            load.wait()
        index = expert(step)
        momentum_block(stack[2], stack[3], step % slots, low_ref, index, sq_ref, index % owners, step // owners)
        store(stack, new_m, out_sem, step).start()

    for step in range(FIRST):
        compute(step, stack2, new_m2, out_sem2, low2, sq2)

    pl.semaphore_wait(barrier, owners - 1)

    def window(x_ref, k, at_model, at_data):
        rows, cols = x_ref.shape[1] // 4, x_ref.shape[2] // 2
        return x_ref.at[k, pl.ds(pl.multiple_of(at_data * rows, rows), rows), pl.ds(pl.multiple_of(at_model * cols, cols), cols)]

    def forward_round(k, computed, stack, new_m, out_sem, low_ref, x_ref, fwd, got, sq_ref, sums_ref, sq_send, sq_got):
        def send(turn):
            place = peer(turn)
            owner = place[0] * 4 + place[1]
            pltpu.make_async_remote_copy(sq_ref.at[owner, k], sums_ref.at[k, me], sq_send.at[k], sq_got.at[k], **at(place)).start()
            pltpu.make_async_remote_copy(low_ref.at[k * owners + owner], window(x_ref, k, model, data), fwd.at[k], got.at[k],
                                         **at(place)).start()

        @pl.loop(0, owners)
        def block(turn):
            step = k * owners + turn

            @pl.when(step >= computed)
            def compute_now():
                compute(step, stack, new_m, out_sem, low_ref, sq_ref)

            @pl.when(turn > 0)
            def send_before():
                send(turn - 1)

            @pl.when(step >= slots - AHEAD)
            def stored():
                store(stack, new_m, out_sem, step + AHEAD - slots).wait()

            @pl.when(step + AHEAD < experts)
            def prefetch():
                for load in loads(stack, step + AHEAD):
                    load.start()

        pltpu.make_async_copy(sq_ref.at[me, k], sums_ref.at[k, me], sq_got.at[k]).start()
        pltpu.make_async_copy(low_ref.at[k * owners + me], window(x_ref, k, model, data), got.at[k]).start()

    def return_round(k, x_ref, dst, sems, t, early, first_column):
        def give(turn):
            place = peer(turn)
            pltpu.make_async_remote_copy(window(x_ref, k, *place), dst.at[k * owners + me], sems.at[k], done_sems.at[t],
                                         **at(place)).start()

        @pl.when(k < early)
        def to_diagonal():
            for turn in range(DIAGONAL):
                give(turn)

        for turn in (2, 4, 3, 5, 6):
            give(turn)
        pltpu.make_async_copy(window(x_ref, k, model, data), dst.at[k * owners + me], done_sems.at[t]).start()

        @pl.when(k >= early)
        def keep():
            cols = dst.shape[2]
            span = pl.ds(pl.multiple_of(first_column + (k - early) * cols, cols), cols)
            pltpu.make_async_copy(window(x_ref, k, *peer(1)), late_a.at[:, span], late_sem.at[0]).start()
            cross = window(x_ref, k, *peer(0))
            last = k == rounds - 1 if t == 0 else False

            @pl.when(jnp.logical_not(last))
            def keep_b():
                pltpu.make_async_copy(cross, late_b.at[:, span], late_sem.at[1]).start()

            if t == 0:
                @pl.when(last)
                def keep_c():
                    pltpu.make_async_copy(cross, late_c, late_sem.at[2]).start()

    def wait_bytes(ref, sem):
        pltpu.make_async_copy(ref, ref, sem).wait()

    def orthogonalize(k, x_ref, got, sums_ref, sq_got, gram_ref, poly_ref):
        wait_bytes(sums_ref.at[k], sq_got.at[k])
        wait_bytes(x_ref.at[k], got.at[k])
        norm = jnp.sqrt(jnp.sum(sums_ref[k])) + NORM_EPS
        rows = x_ref.shape[1]

        @pl.loop(0, rows // 256)
        def normalize(i):
            span = pl.ds(pl.multiple_of(i * 256, 256), 256)
            x_ref[k, span, :] = (x_ref[k, span, :].astype(jnp.float32) / norm).astype(jnp.bfloat16)

        iterate(x_ref.at[k], gram_ref, poly_ref)

    @pl.loop(0, rounds)
    def forward(k):
        forward_round(k, FIRST, stack2, new_m2, out_sem2, low2, x2, fwd2, got2, sq2, sums2, sq_send2, sq_got2)
        forward_round(k, 0, stack1, new_m1, out_sem1, low1, x1, fwd1, got1, sq1, sums1, sq_send1, sq_got1)

    cols1, cols2 = low1.shape[2], low2.shape[2]

    @pl.loop(0, rounds)
    def work(k):
        orthogonalize(k, x2, got2, sums2, sq_got2, gram2, poly2)
        return_round(k, x2, back2, ret2, 0, early2, LATE[0] * cols1)
        orthogonalize(k, x1, got1, sums1, sq_got1, gram1, poly1)
        return_round(k, x1, back1, ret1, 1, early1, 0)

    count = owners - 1
    for stack, new_m, out_sem in ((stack2, new_m2, out_sem2), (stack1, new_m1, out_sem1)):
        for step in range(experts + AHEAD - slots, experts):
            store(stack, new_m, out_sem, step).wait()

    @pl.loop(0, rounds)
    def finish(k):
        for low, sq, fwd, ret, sq_send, early in ((low2, sq2, fwd2, ret2, sq_send2, early2), (low1, sq1, fwd1, ret1, sq_send1, early1)):
            wait_bytes(sq.at[pl.ds(0, count), 0], sq_send.at[k])
            wait_bytes(low.at[pl.ds(0, count)], fwd.at[k])

            wait_bytes(low.at[pl.ds(0, count - DIAGONAL)], ret.at[k])

            @pl.when(k < early)
            def returned():
                wait_bytes(low.at[pl.ds(0, DIAGONAL)], ret.at[k])

    wait_bytes(back2.at[pl.ds(0, experts - LATE[1] * DIAGONAL)], done_sems.at[0])
    wait_bytes(back1.at[pl.ds(0, experts - LATE[0] * DIAGONAL)], done_sems.at[1])
    wait_bytes(late_a, late_sem.at[0])
    wait_bytes(late_b, late_sem.at[1])
    wait_bytes(late_c, late_sem.at[2])


def exchange(m1, g1, m2, g2, owners):
    experts, rows, cols1 = m1.shape
    cols2 = m2.shape[2]
    rounds = experts // owners
    slots = 2 * AHEAD
    any_spec = pl.BlockSpec(memory_space=pl.ANY)
    flops = 2 * rounds * NS_STEPS * sum(2 * 4 * rows * c * c + c ** 3 for c in (2 * cols1, 2 * cols2))
    low = jnp.bfloat16
    dma = pltpu.SemaphoreType.DMA
    results = [((experts, rows, cols1), jnp.float32), ((experts, rows, cols2), jnp.float32),
               ((experts, rows, cols1), low), ((experts, rows, cols2), low),
               ((rows, LATE[0] * cols1 + LATE[1] * cols2), low), ((rows, LATE[0] * cols1 + (LATE[1] - 1) * cols2), low),
               ((rows, cols2), low)]
    return pl.pallas_call(
        exchange_kernel,
        in_specs=[any_spec] * 4,
        out_specs=[any_spec] * len(results),
        out_shape=[jax.ShapeDtypeStruct(*result) for result in results],
        scratch_shapes=[
            pltpu.VMEM((experts, rows, cols1), low),
            pltpu.VMEM((experts, rows, cols2), low),
            pltpu.VMEM((rounds, 4 * rows, 2 * cols1), low),
            pltpu.VMEM((rounds, 4 * rows, 2 * cols2), low),
            pltpu.VMEM((owners, rounds, 8, 128), jnp.float32),
            pltpu.VMEM((owners, rounds, 8, 128), jnp.float32),
            pltpu.VMEM((rounds, owners, 8, 128), jnp.float32),
            pltpu.VMEM((rounds, owners, 8, 128), jnp.float32),
            pltpu.VMEM((2 * cols1, 2 * cols1), low),
            pltpu.VMEM((2 * cols1, 2 * cols1), low),
            pltpu.VMEM((2 * cols2, 2 * cols2), low),
            pltpu.VMEM((2 * cols2, 2 * cols2), low),
            pltpu.VMEM((slots, rows, cols1), jnp.float32),
            pltpu.VMEM((slots, rows, cols1), low),
            pltpu.VMEM((slots, rows, cols2), jnp.float32),
            pltpu.VMEM((slots, rows, cols2), low),
        ] + [dma((rounds,))] * 6 + [dma((2,))] + [dma((rounds,))] * 4 + [dma((slots,))] * 6 + [dma((3,))],
        compiler_params=pltpu.CompilerParams(collective_id=0, has_side_effects=True, vmem_limit_bytes=62 * 2 ** 20),
        cost_estimate=pl.CostEstimate(flops=flops, bytes_accessed=14 * (m1.size + m2.size), transcendentals=0),
        name='exchange',
    )(m1, g1, m2, g2)


def call_plain(kernel, name, steps, in_specs, out_specs, out_shape, place, args, aliases, traffic, limit):
    return pl.pallas_call(
        kernel,
        grid_spec=pltpu.PrefetchScalarGridSpec(num_scalar_prefetch=1, grid=(steps,), in_specs=in_specs, out_specs=out_specs),
        out_shape=out_shape, input_output_aliases=aliases,
        compiler_params=pltpu.CompilerParams(dimension_semantics=('arbitrary',), vmem_limit_bytes=limit * 2 ** 20),
        cost_estimate=pl.CostEstimate(flops=traffic, bytes_accessed=traffic, transcendentals=0),
        name=name,
    )(place, *args)


def weight_block(w_ref, x_mat, out_ref, scale):
    w_old = w_ref[...]
    out_ref[...] = w_old - LEARN_RATE * (x_mat.astype(jnp.float32) * scale + DECAY * w_old)


def early_kernel(scales, place, m1_ref, m2_ref, w1_ref, w2_ref, x1_ref, x2_ref, new_m1_ref, new_m2_ref, new_w1_ref, new_w2_ref):
    new_m1_ref[...] = m1_ref[...]
    new_m2_ref[...] = m2_ref[...]
    weight_block(w1_ref, x1_ref[...], new_w1_ref, scales[0])
    weight_block(w2_ref, x2_ref[...], new_w2_ref, scales[1])


def early_step(m1, m2, w1, w2, x1, x2, scales, pair, owners):
    steps, pairs = m1.shape[0] // 2, owners // 2

    def spec(array, late):
        def turn(i, place):
            other = (place[0] + 1 + jnp.minimum(i % pairs, pairs - 2)) % pairs
            return jnp.where(i < steps - late * pairs, i, i // pairs * pairs + other), 0, 0

        return pl.BlockSpec((2,) + array.shape[1:], turn)

    m_specs = [pl.BlockSpec((2,) + m.shape[1:], lambda i, place: (i, 0, 0)) for m in (m1, m2)]
    w_specs = [spec(w, late) for w, late in zip((w1, w2), LATE)]
    outs = [jax.ShapeDtypeStruct(array.shape, array.dtype) for array in (m1, m2, w1, w2)]
    traffic = 18 * (m1.size + m2.size)
    return call_plain(functools.partial(early_kernel, scales), 'early', steps, m_specs + w_specs + w_specs, m_specs + w_specs,
                      outs, pair, (m1, m2, w1, w2, x1, x2), {}, traffic, 60)


def late_kernel(scales, jobs, given, keep, place, w1_ref, w2_ref, *refs):
    given_refs, refs = refs[:given], refs[given:]
    sources, refs = refs[:len(jobs)], refs[len(jobs) + 2:]
    outs, kept, refs = refs[:2], refs[2:2 + len(keep)], refs[2 + len(keep):]
    bufs, (load_sems, store_sems, keep_sem) = refs[:2], refs[2:]
    w_refs = w1_ref, w2_ref
    keeps = [pltpu.make_async_copy(w_refs[stack].at[first_expert + (place[0] ^ which)], ref.at[0], keep_sem)
             for (stack, first_expert, which), ref in zip(keep, kept)]
    work, used = [], [0, 0]
    for (which, blocks), source in zip(jobs, sources):
        for stack, first_expert, column in blocks:
            slot = used[stack]
            used[stack] += 1
            index = first_expert + (place[0] ^ which)
            buf = bufs[stack].at[slot]
            load = None if given else pltpu.make_async_copy(w_refs[stack].at[index], buf, load_sems.at[stack, slot])
            if load is not None:
                load.start()
            work.append((load, pltpu.make_async_copy(buf, outs[stack].at[index], store_sems.at[stack, slot]),
                         buf, source.at[:, pl.ds(column, buf.shape[1])], scales[stack]))
    for copy in keeps:
        copy.start()
    for load, store, buf, x_ref, scale in work:
        if load is not None:
            load.wait()
        weight_block(given_refs[0].at[0] if given else buf, x_ref[...], buf, scale)
        store.start()
    for _, store, _, _, _ in work:
        store.wait()
    for copy in keeps:
        copy.wait()


def late_step(w1, w2, into1, into2, scales, place, jobs, given=(), keep=()):
    any_spec, vmem_spec = pl.BlockSpec(memory_space=pl.ANY), pl.BlockSpec(memory_space=pltpu.VMEM)
    count = [max(1, sum(block[0] == stack for job in jobs for block in job[2])) for stack in range(2)]
    held = [pltpu.with_memory_space_constraint(w, pltpu.HBM) for w in (w1, w2)]
    arrays = [job[0] for job in jobs]
    traffic = 5 * sum(array.size for array in arrays)
    before = 3 + len(given) + len(jobs)
    return pl.pallas_call(
        functools.partial(late_kernel, scales, [job[1:] for job in jobs], len(given), keep),
        in_specs=[pl.BlockSpec(memory_space=pltpu.SMEM)] + [any_spec] * 2 + [vmem_spec] * (before - 3) + [any_spec] * 2,
        out_specs=[any_spec] * (2 + len(keep)),
        out_shape=[jax.ShapeDtypeStruct(w.shape, w.dtype) for w in (w1, w2)]
        + [jax.ShapeDtypeStruct((1,) + (w1, w2)[stack].shape[1:], w1.dtype) for stack, _, _ in keep],
        scratch_shapes=[pltpu.VMEM((n,) + w.shape[1:], w.dtype) for n, w in zip(count, (w1, w2))]
        + [pltpu.SemaphoreType.DMA((2, max(count)))] * 2 + [pltpu.SemaphoreType.DMA],
        input_output_aliases={before: 0, before + 1: 1},
        compiler_params=pltpu.CompilerParams(vmem_limit_bytes=24 * 2 ** 20),
        cost_estimate=pl.CostEstimate(flops=traffic, bytes_accessed=2 * traffic, transcendentals=0),
        name='late',
    )(place, *held, *given, *arrays, into1, into2)


def solution(mesh):
    data_size = mesh.shape['data']
    model_size = mesh.shape['model']
    owners = data_size * model_size
    block_spec = P('stage', 'data', 'model')

    def local_step(w_fc1, m_fc1, g_fc1, w_fc2, m_fc2, g_fc2):
        scales = [0.2 * math.sqrt(max(w.shape[1] * data_size, w.shape[2] * model_size)) for w in (w_fc1, w_fc2)]
        model, data = lax.axis_index('model'), lax.axis_index('data')
        pair = 3 - model * 2 - (data >> 1)
        same = pair * 2 + (data & 1)
        new_m1, new_m2, back1, back2, late_a, late_b, late_c = exchange(m_fc1, g_fc1, m_fc2, g_fc2, owners)
        late_a = lax.ppermute(late_a, ('model', 'data'), [(i, i ^ 6) for i in range(owners)])
        late_b = lax.ppermute(late_b, ('model', 'data'), [(i, i ^ 7) for i in range(owners)])
        late_c = lax.ppermute(late_c, ('model', 'data'), [(i, i ^ 7) for i in range(owners)])
        new_m1, new_m2, new_w1, new_w2 = early_step(new_m1, new_m2, w_fc1, w_fc2, back1, back2, scales, pair[None], owners)
        experts, (cols1, cols2) = w_fc1.shape[0], (w_fc1.shape[2], w_fc2.shape[2])
        blocks = [(0, experts - (LATE[0] - i) * owners, i * cols1) for i in range(LATE[0])]
        blocks += [(1, experts - (LATE[1] - i) * owners, LATE[0] * cols1 + i * cols2) for i in range(LATE[1])]
        new_w1, new_w2, w_last = late_step(w_fc1, w_fc2, new_w1, new_w2, scales, same[None],
                                           [(late_a, 0, blocks), (late_b, 1, blocks[:-1])], keep=[(1, experts - owners, 1)])
        new_w1, new_w2 = late_step(w_fc1, w_fc2, new_w1, new_w2, scales, same[None],
                                   [(late_c, 1, [(1, experts - owners, 0)])], given=[w_last])
        return new_w1, new_m1, new_w2, new_m2

    return jax.shard_map(local_step, mesh=mesh, in_specs=(block_spec,) * 6, out_specs=(block_spec,) * 4, check_vma=False)
```
